256 devices in a mesh: horizon: 32 (over z, x), batch: 8 (over y, core).
Axes of the slice: x: 4, y: 4, z: 8, core: 2. Of those that a mesh axis runs over, the one named last changes fastest.
Arguments:
- dynamics: float32 [8, 256, 48, 48], P('batch', 'horizon'), may hold values from -0.1 to 1.1
- inputs: float32 [8, 256, 48, 16], P('batch', 'horizon'), may hold values from -0.6 to 0.6
- state_cost: float32 [8, 256, 48, 48], P('batch', 'horizon'), may hold values from -1 to 1, as said below
- input_cost: float32 [8, 256, 16, 16], P('batch', 'horizon'), may hold values from -0.2 to 2.2, as said below
- drift: float32 [8, 256, 48], P('batch', 'horizon'), may hold values from -0.6 to 0.6
- target: float32 [8, 256, 48], P('batch', 'horizon'), may hold values from -6 to 6
- initial: float32 [8, 48], P('batch'), may hold values from -6 to 6
Outputs:
- hessian: float32 [8, 4096, 4096], P('batch', 'horizon')
- gradient: float32 [8, 4096], P('batch', 'horizon')
The draws below stay inside these ranges and needn't reach their ends.
Inputs may be any that keep to these rules, and one draw needn't show every extreme that they name: `state_cost`: each 48 x 48 matrix is symmetric and positive definite. `input_cost`: each 16 x 16 matrix is symmetric and positive definite.
All inputs are finite; a program needn't handle non-finite values.
Results may differ from the reference program's by a relative error of at most 0.0003.
Values sent between devices are 32-bit elements; how exact they have to be, the bound alone decides.
A program may use at most 128 MiB of HBM per device.

```python
import math
import jax
import jax.numpy as jnp
from jax import lax

NX = 48
NU = 16
INTERVAL_TOTAL = 256
TASK_TOTAL = 8


def draw_dynamics(key, part):
    seed_handles = jax.random.split(jax.random.fold_in(key, 11), 4)
    lowest, highest = (0.5, 12.0)
    expansion_speed = jnp.exp(jax.random.uniform(seed_handles[0], (TASK_TOTAL, 1, NX), jnp.float32, math.log(lowest), math.log(highest))) / INTERVAL_TOTAL
    dispersion_span = jnp.exp(jax.random.uniform(seed_handles[1], (TASK_TOTAL, INTERVAL_TOTAL, NX), jnp.float32, math.log(0.5), math.log(2.0)))
    spike_magnitude = jnp.where(jax.random.uniform(seed_handles[2], (TASK_TOTAL, INTERVAL_TOTAL, 1), jnp.float32) < 4.0 / INTERVAL_TOTAL, 0.6, 1.0)
    damping_multiplier = jnp.exp(-expansion_speed * dispersion_span) * spike_magnitude
    noise = jnp.clip(jax.random.normal(seed_handles[3], (TASK_TOTAL, INTERVAL_TOTAL, NX, NX), jnp.float32), -4.0, 4.0) * (0.2 / NX)
    return noise + damping_multiplier[..., None] * jnp.eye(NX, dtype=jnp.float32)


def draw_state_cost(key, part):
    seed_handles = jax.random.split(jax.random.fold_in(key, 23), 2)
    lowest, highest = (2.0, 20.0)
    divisor = float(max(INTERVAL_TOTAL, 48))
    diagonal = jnp.exp(jax.random.uniform(seed_handles[0], (TASK_TOTAL, INTERVAL_TOTAL, NX), jnp.float32, math.log(lowest), math.log(highest))) / divisor
    raw = jnp.clip(jax.random.normal(seed_handles[1], (TASK_TOTAL, INTERVAL_TOTAL, NX, NX), jnp.float32), -4.0, 4.0) * (0.1 / divisor)
    symmetric = (raw + jnp.swapaxes(raw, -1, -2)) * 0.7071
    return symmetric + diagonal[..., None] * jnp.eye(NX, dtype=jnp.float32)


def draw_input_cost(key, part):
    seed_handles = jax.random.split(jax.random.fold_in(key, 37), 2)
    diagonal = jnp.exp(jax.random.uniform(seed_handles[0], (TASK_TOTAL, INTERVAL_TOTAL, NU), jnp.float32, math.log(0.5), math.log(2.0)))
    raw = jnp.clip(jax.random.normal(seed_handles[1], (TASK_TOTAL, INTERVAL_TOTAL, NU, NU), jnp.float32), -4.0, 4.0) * 0.03
    symmetric = (raw + jnp.swapaxes(raw, -1, -2)) * 0.7071
    return symmetric + diagonal[..., None] * jnp.eye(NU, dtype=jnp.float32)


def steps_of(rng, dims, shards, least, largest):
    gain = 1.0
    for axis_at, blocks in shards:
        heights = jax.random.uniform(jax.random.fold_in(jax.random.fold_in(rng, 6), axis_at), (blocks,), jnp.float32, least / len(shards), largest / len(shards))
        gain = gain * jnp.repeat(jnp.exp(heights), dims[axis_at] // blocks).reshape((-1,) + (1,) * (len(dims) - 1 - axis_at))
    return gain


def centred(stream_key, shape, scale, bound, pieces=(), kind=jnp.bfloat16):
    values = scale * jax.random.normal(stream_key, shape, jnp.float32)
    if pieces:
        values = values * steps_of(stream_key, shape, pieces, -0.22, 0.18)
    return jnp.clip(values, -bound, bound).astype(kind)


def setup_inputs(seed: int = 0) -> dict:
    arg_keys = jax.random.split(jax.random.key(seed), 8)
    return {
        "dynamics": draw_dynamics(jax.random.fold_in(arg_keys[7], 71), 0),
        "inputs": centred(arg_keys[1], (TASK_TOTAL, INTERVAL_TOTAL, NX, NU), 0.1, 0.6, ((0, 8), (1, 32)), jnp.float32),
        "state_cost": draw_state_cost(jax.random.fold_in(arg_keys[7], 71), 0),
        "input_cost": draw_input_cost(jax.random.fold_in(arg_keys[7], 71), 0),
        "drift": centred(arg_keys[4], (TASK_TOTAL, INTERVAL_TOTAL, NX), 0.1, 0.6, ((0, 8), (1, 32)), jnp.float32),
        "target": centred(arg_keys[5], (TASK_TOTAL, INTERVAL_TOTAL, NX), 1.0, 6.0, ((0, 8), (1, 32)), jnp.float32),
        "initial": centred(arg_keys[6], (TASK_TOTAL, NX), 1.0, 6.0, ((0, 8),), jnp.float32),
    }


HI = lax.Precision.HIGHEST


def condense_one(items):
    section_dynamics, section_inputs, section_costs, section_input_costs, section_drift, section_target, start = items
    width = INTERVAL_TOTAL * NU

    def roll_states(state, parts):
        matrix, shift_vec, goal, weight = parts
        after = jnp.dot(matrix, state, precision=HI) + shift_vec
        return after, jnp.dot(weight, after - goal, precision=HI)

    _, weighted = lax.scan(roll_states, start, (section_dynamics, section_drift, section_target, section_costs))

    def sweep_costs(tail, parts):
        matrix, weight = parts
        total_cost = weight + tail
        return jnp.dot(matrix.T, jnp.dot(total_cost, matrix, precision=HI), precision=HI), total_cost

    _, cost_to_go = lax.scan(sweep_costs, jnp.zeros((NX, NX), jnp.float32), (section_dynamics, section_costs), reverse=True)
    values = jnp.einsum("sij,sjk->sik", cost_to_go, section_inputs, precision=HI)

    def sweep_columns(carry, parts):
        block, vector = carry
        matrix, control, value, weight, index = parts
        row_block = jnp.dot(control.T, block, precision=HI)
        summed = weight + vector
        grad_block = jnp.dot(control.T, summed, precision=HI)
        placed = lax.dynamic_update_slice_in_dim(block, value, (index * NU).astype(jnp.int32), 1)
        return (jnp.dot(matrix.T, placed, precision=HI), jnp.dot(matrix.T, summed, precision=HI)), (row_block, grad_block)

    indices = jnp.arange(INTERVAL_TOTAL, dtype=jnp.int32)
    start_carry = (jnp.zeros((NX, width), jnp.float32), jnp.zeros((NX,), jnp.float32))
    _, (row_blocks, grad_blocks) = lax.scan(sweep_columns, start_carry, (section_dynamics, section_inputs, values, weighted, indices), reverse=True)
    upper = row_blocks.reshape(width, width)
    diagonal_blocks = jnp.einsum("sji,sjk->sik", section_inputs, values, precision=HI) + section_input_costs
    block_diag = jnp.einsum("st,sij->sitj", jnp.eye(INTERVAL_TOTAL, dtype=jnp.float32), diagonal_blocks, precision=HI).reshape(width, width)
    return upper + upper.T + block_diag, grad_blocks.reshape(width)


def reference(dynamics, inputs, state_cost, input_cost, drift, target, initial):
    hessian, gradient = lax.map(condense_one, (dynamics, inputs, state_cost, input_cost, drift, target, initial))
    return (hessian, gradient)
```

```python
import functools

import jax
import jax.numpy as jnp
from jax import lax
from jax.experimental import pallas as pl
from jax.experimental.pallas import tpu as pltpu
from jax.sharding import PartitionSpec as P

NX = 48
NU = 16
SEC = 8
COLS = SEC * NU
GX = 4
GZ = 8
F32 = jnp.float32
BF16 = jnp.bfloat16
Z_ORDER = (4, 3, 5, 2, 6, 1, 7)
ARRIVE = (1, 7, 2, 6, 3, 5, 4)


def split(a):
    high = a.astype(BF16)
    return high, (a - high.astype(F32)).astype(BF16)


def dot(a, b):
    return lax.dot_general(a, b, (((1,), (0,)), ((), ())), preferred_element_type=F32)


def mm(a, b):
    ah, al = split(a)
    bh, bl = split(b)
    return dot(ah, bh) + (dot(ah, bl) + dot(al, bh))


def sq(a):
    return a[:, :NX]


def transposed(a):
    return jnp.transpose(jnp.concatenate([a, jnp.zeros((128 - a.shape[0], 128), F32)], axis=0))


def body(
    a_hbm, b_hbm, q_hbm, r_hbm, d_hbm, t_hbm, i_hbm,
    h_ref, grad_ref,
    a_v, b_v, q_v, r_v, d_v, t_v, i_v,
    y_v, qy_v, x_tc, x_lr, z_tc, z_l, z_r, coef_a, coef_b, rhs,
    in_sem, xt_s, xt_r, xl_s, xl_r, zt_s, zt_r, zl_s, zl_r, zr_s, zr_r, w_s, w_r,
):
    me = lax.axis_index("horizon")
    z, x = me // GX, me % GX

    loads = [
        pltpu.make_async_copy(src.at[0], dst, in_sem.at[k])
        for k, (src, dst) in enumerate(
            ((a_hbm, a_v), (b_hbm, b_v), (d_hbm, d_v), (t_hbm, t_v), (q_hbm, q_v), (r_hbm, r_v))
        )
    ]
    loads.append(pltpu.make_async_copy(i_hbm, i_v, in_sem.at[6]))
    for load in loads:
        load.start()

    for g in range(GZ):
        z_r[g] = jnp.zeros((NX, COLS), F32)

    def x_peer(d):
        return z * GX + (x + d) % GX

    def z_peer(d):
        return ((z + d) % GZ) * GX + x

    barrier = pltpu.get_barrier_semaphore()
    for d in range(1, GX):
        pl.semaphore_signal(barrier, inc=1, device_id={"horizon": x_peer(d)}, device_id_type=pl.DeviceIdType.MESH)
    for d in range(1, GZ):
        pl.semaphore_signal(barrier, inc=1, device_id={"horizon": z_peer(d)}, device_id_type=pl.DeviceIdType.MESH)

    def remote(ref, send, recv, peer):
        return pltpu.make_async_remote_copy(
            src_ref=ref, dst_ref=ref, send_sem=send, recv_sem=recv,
            device_id={"horizon": peer}, device_id_type=pl.DeviceIdType.MESH,
        )

    for load in loads:
        load.wait()

    lane = lax.broadcasted_iota(jnp.int32, (NX, 128), 1)
    row = lax.broadcasted_iota(jnp.int32, (NX, 128), 0)
    unit = jnp.where(lane == row, 1.0, 0.0).astype(F32)

    vectors = jnp.concatenate(
        [
            jnp.concatenate([d_v[...], t_v[...], jnp.broadcast_to(i_v[...], (8, NX))], axis=0),
            jnp.zeros((24, 128 - NX), F32),
        ],
        axis=1,
    )
    columns = transposed(vectors)[:NX]

    def vector_at(k):
        return jnp.where(lane == NX, pltpu.roll(columns, (NX - k) % 128, 1), 0.0)

    wide = jnp.zeros((NX, 128 - NX), F32)
    state = None
    for t in range(SEC):
        entry = vector_at(t)
        placed = jnp.concatenate([b_v[t], jnp.zeros((NX, 128 - NU), F32)], axis=1)
        if t:
            placed = pltpu.roll(placed, NU * t, 1)
        added = jnp.concatenate([entry, placed], axis=1)
        if t == 0:
            state = added + jnp.concatenate([a_v[0], wide, jnp.zeros((NX, 128), F32)], axis=1)
        else:
            state = mm(a_v[t], state) + added
        error = jnp.concatenate([state[:, :128] - vector_at(SEC + t), state[:, 128:]], axis=1)
        y_v[NX * t : NX * (t + 1), :] = error
        qy_v[NX * t : NX * (t + 1), :] = mm(q_v[t], error)
    gram = mm(jnp.transpose(y_v[...]), qy_v[...])
    own_l = state[:, 128:]
    own_r = gram[:NX, 128:]
    own_t = sq(state)
    x_tc[x] = state[:, :128] + pltpu.roll(gram[:NX, :128], 64, 1)
    x_lr[x, 0] = own_l
    x_lr[x, 1] = own_r

    pl.semaphore_wait(barrier, GX - 1 + GZ - 1)
    sends = []

    def send(ref, s, r, peer):
        copy = remote(ref, s, r, peer)
        copy.start()
        sends.append(copy)

    for d in (2, 1, 3):
        send(x_tc.at[x], xt_s.at[d], xt_r.at[x], x_peer(d))
    for d in (2, 1, 3):
        send(x_lr.at[x], xl_s.at[d], xl_r.at[x], x_peer(d))

    for d in range(1, GX):
        i = (x + d) % GX
        remote(x_tc.at[i], xt_s.at[d], xt_r.at[i], x_peer(d)).wait_recv()

    def unpack(packed):
        maps, costs = [], []
        for i in range(packed.shape[0]):
            both = packed[i]
            maps.append(jnp.where(lane < 64, both, 0.0))
            costs.append(jnp.where(lane < 64, pltpu.roll(both, 64, 1), 0.0))
        return maps, costs, [transposed(m)[:NX] for m in maps]

    def fold(tail, m, c, mt):
        inner = mm(sq(tail), m) + jnp.where(lane == NX, tail, 0.0)
        return c + mm(sq(mt), inner)

    def choose(index, values):
        out = values[0]
        for k in range(1, len(values)):
            out = jnp.where(index == k, values[k], out)
        return out

    nothing = jnp.zeros((NX, 128), F32)

    xm, xc, xmt = unpack(x_tc)
    tails = [None] * GX
    tail = nothing
    for i in reversed(range(GX)):
        tails[i] = tail
        tail = fold(tail, xm[i], xc[i], xmt[i])
    group_cost = tail
    before = [unit]
    for i in range(GX):
        if i == 0:
            before.append(xm[0])
        else:
            before.append(mm(sq(xm[i]), before[i]) + jnp.where(lane == NX, xm[i], 0.0))
    after = [None] * GX
    after[GX - 1] = unit
    after[GX - 2] = jnp.where(lane < NX, xm[GX - 1], 0.0)
    for i in reversed(range(GX - 2)):
        after[i] = mm(sq(after[i + 1]), jnp.where(lane < NX, xm[i + 1], 0.0))
    group_map = before[GX]
    own_mt = choose(x, xmt)
    own_before = choose(x, before[:GX])
    own_before_t = transposed(jnp.where(lane < NX, own_before, 0.0))[:NX]
    group_l = mm(sq(choose(x, after)), own_l)
    group_r = mm(
        sq(own_before_t), own_r + mm(sq(own_mt), mm(sq(choose(x, tails)), own_l))
    )
    z_tc[z] = group_map + pltpu.roll(group_cost, 64, 1)
    z_l[z] = group_l
    z_r[z] = group_r

    for d in Z_ORDER:
        send(z_tc.at[z], zt_s.at[d], zt_r.at[z], z_peer(d))
    for d in Z_ORDER:
        send(z_l.at[z], zl_s.at[d], zl_r.at[z], z_peer(d))
    for d in Z_ORDER:
        @pl.when((z + d) % GZ < z)
        def _():
            remote(z_r.at[z], zr_s.at[d], zr_r.at[z], z_peer(d)).start()

    for d in range(1, GZ):
        g = (z + d) % GZ
        remote(z_tc.at[g], zt_s.at[d], zt_r.at[g], z_peer(d)).wait_recv()

    zm, zc, zmt = unpack(z_tc)
    tail = nothing
    z_tails = [None] * GZ
    for g in reversed(range(GZ)):
        z_tails[g] = tail
        if g:
            tail = fold(tail, zm[g], zc[g], zmt[g])
    carry = unit
    backs = []
    for g in range(GZ):
        nxt = carry if g == 0 else jnp.where(g > z + 1, mm(sq(carry), zmt[g - 1]), unit)
        backs.append(jnp.where(lane < NX, nxt, 0.0))
        carry = backs[g]
    backs.append(jnp.where(lane < NX, mm(sq(carry), zmt[GZ - 1]), 0.0))
    carry = unit
    fronts = [None] * GZ
    for g in reversed(range(GZ)):
        fronts[g] = carry if g == GZ - 1 else jnp.where(g < z - 1, mm(sq(carry), zm[g + 1]), unit)
        carry = jnp.where(lane < NX, fronts[g], 0.0)
        fronts[g] = carry
    for g in range(GZ):
        coef_a[g] = jnp.where(g > z, backs[g], nothing)
        coef_b[g] = jnp.where(g > z, mm(sq(backs[g + 1]), z_tails[g]), fronts[g])
    enter = vector_at(2 * SEC)
    for g in range(GZ - 1):
        enter = jnp.where(g < z, mm(sq(zm[g]), enter) + jnp.where(lane == NX, zm[g], 0.0), enter)
    group_tail = choose(z, z_tails)

    for d in ARRIVE:
        g = (z + d) % GZ
        remote(z_l.at[g], zl_s.at[d], zl_r.at[g], z_peer(d)).wait_recv()

        @pl.when(g > z)
        def _():
            remote(z_r.at[g], zr_s.at[d], zr_r.at[g], z_peer(d)).wait_recv()

        rhs[g, x] = mm(sq(coef_a[g]), z_r[g]) + mm(sq(coef_b[g]), z_l[g])
        for e in range(1, GX):
            send(rhs.at[g, x], w_s.at[d, e], w_r.at[g, x], x_peer(e))

    for d in range(1, GX):
        i = (x + d) % GX
        remote(x_lr.at[i], xl_s.at[d], xl_r.at[i], x_peer(d)).wait_recv()
    tail = group_tail
    for i in reversed(range(GX)):
        tails[i] = tail
        if i:
            tail = fold(tail, xm[i], xc[i], xmt[i])
    own_tail = choose(x, tails)
    carry = unit
    backs = []
    for i in range(GX):
        nxt = carry if i == 0 else jnp.where(i > x + 1, mm(sq(carry), xmt[i - 1]), unit)
        backs.append(jnp.where(lane < NX, nxt, 0.0))
        carry = backs[i]
    backs.append(jnp.where(lane < NX, mm(sq(carry), xmt[GX - 1]), 0.0))
    carry = unit
    for i in reversed(range(GX)):
        front = carry if i == GX - 1 else jnp.where(i < x - 1, mm(sq(carry), xm[i + 1]), unit)
        carry = jnp.where(lane < NX, front, 0.0)
        ca = jnp.where(i > x, backs[i], nothing)
        cb = jnp.where(i > x, mm(sq(backs[i + 1]), tails[i]), jnp.where(i == x, own_tail, carry))
        rhs[z, i] = mm(sq(ca), x_lr[i, 1]) + mm(sq(cb), x_lr[i, 0])

    entering = mm(sq(own_before), enter) + jnp.where((lane == NX) & (x > 0), own_before, 0.0)
    leaving = mm(own_t, entering) + jnp.where(lane == NX, state[:, :128], 0.0)
    costate = mm(sq(own_tail), leaving) + jnp.where(lane == NX, own_tail, 0.0)
    grad_ref[...] = gram[NX : NX + 1, 128:] + jnp.sum(
        entering[:, NX : NX + 1] * own_r + costate[:, NX : NX + 1] * own_l, axis=0, keepdims=True
    )

    full_r = own_r + mm(sq(own_mt), mm(sq(own_tail), own_l))
    group_mt = transposed(jnp.where(lane < NX, group_map, 0.0))[:NX]
    group_full = group_r + mm(sq(group_mt), mm(sq(group_tail), group_l))

    def factors(value):
        high, low = split(value)
        turned = jnp.transpose(
            jnp.concatenate([high.astype(F32), low.astype(F32), jnp.zeros((32, 128), F32)], axis=0)
        )
        return turned.astype(BF16)[:, : 2 * NX]

    def rows(left, right):
        high, low = split(right)
        return dot(left, jnp.concatenate([high, high], axis=0)) + dot(left[:, :NX], low)

    f_gl, f_gr = factors(group_l), factors(group_full)
    f_l, f_r = factors(own_l), factors(full_r)

    tile = gram[128:, 128:]
    cost = jnp.concatenate(
        [
            jnp.concatenate([r_v[t], jnp.zeros((NU, 128 - NU), F32)], axis=1)
            if t == 0
            else pltpu.roll(jnp.concatenate([r_v[t], jnp.zeros((NU, 128 - NU), F32)], axis=1), NU * t, 1)
            for t in range(SEC)
        ],
        axis=0,
    )
    for i in range(GX):
        left = jnp.where(i < x, f_r.astype(F32), f_l.astype(F32)).astype(BF16)
        block = rows(left, rhs[z, i])
        block = block + jnp.where(i == x, tile + cost, 0.0)
        h_ref[:, pl.ds(pl.multiple_of(z * (GX * COLS) + i * COLS, COLS), COLS)] = block

    for d in ARRIVE:
        g = (z + d) % GZ
        left = jnp.where(g > z, f_gl.astype(F32), f_gr.astype(F32)).astype(BF16)
        for e in range(1, GX):
            i = (x + e) % GX
            remote(rhs.at[g, i], w_s.at[d, e], w_r.at[g, i], x_peer(e)).wait_recv()
        right = jnp.concatenate([rhs[g, i] for i in range(GX)], axis=1)
        h_ref[:, pl.ds(pl.multiple_of(g * (GX * COLS), GX * COLS), GX * COLS)] = rows(left, right)

    for copy in sends:
        copy.wait_send()
    for d in Z_ORDER:
        @pl.when((z + d) % GZ < z)
        def _():
            remote(z_r.at[z], zr_s.at[d], zr_r.at[z], z_peer(d)).wait_send()


def condense(dynamics, inputs, state_cost, input_cost, drift, target, initial):
    dma = pltpu.SemaphoreType.DMA
    hessian, gradient = pl.pallas_call(
        body,
        out_shape=(
            jax.ShapeDtypeStruct((COLS, GX * GZ * COLS), F32),
            jax.ShapeDtypeStruct((1, COLS), F32),
        ),
        in_specs=[pl.BlockSpec(memory_space=pl.ANY)] * 7,
        out_specs=(
            pl.BlockSpec(memory_space=pltpu.VMEM),
            pl.BlockSpec(memory_space=pltpu.VMEM),
        ),
        scratch_shapes=[
            pltpu.VMEM((SEC, NX, NX), F32),
            pltpu.VMEM((SEC, NX, NU), F32),
            pltpu.VMEM((SEC, NX, NX), F32),
            pltpu.VMEM((SEC, NU, NU), F32),
            pltpu.VMEM((SEC, NX), F32),
            pltpu.VMEM((SEC, NX), F32),
            pltpu.VMEM((1, NX), F32),
            pltpu.VMEM((SEC * NX, 256), F32),
            pltpu.VMEM((SEC * NX, 256), F32),
            pltpu.VMEM((GX, NX, 128), F32),
            pltpu.VMEM((GX, 2, NX, COLS), F32),
            pltpu.VMEM((GZ, NX, 128), F32),
            pltpu.VMEM((GZ, NX, COLS), F32),
            pltpu.VMEM((GZ, NX, COLS), F32),
            pltpu.VMEM((GZ, NX, 128), F32),
            pltpu.VMEM((GZ, NX, 128), F32),
            pltpu.VMEM((GZ, GX, NX, COLS), F32),
            dma((7,)),
            dma((GX,)), dma((GX,)), dma((GX,)), dma((GX,)),
            dma((GZ,)), dma((GZ,)), dma((GZ,)), dma((GZ,)), dma((GZ,)), dma((GZ,)),
            dma((GZ, GX)), dma((GZ, GX)),
        ],
        compiler_params=pltpu.CompilerParams(collective_id=0, has_side_effects=True),
        name="condense",
    )(dynamics, inputs, state_cost, input_cost, drift, target, initial)
    return hessian[None], gradient


def solution(mesh):
    return jax.shard_map(
        condense,
        mesh=mesh,
        in_specs=(
            P("batch", "horizon", None, None),
            P("batch", "horizon", None, None),
            P("batch", "horizon", None, None),
            P("batch", "horizon", None, None),
            P("batch", "horizon", None),
            P("batch", "horizon", None),
            P("batch", None),
        ),
        out_specs=(P("batch", "horizon", None), P("batch", "horizon")),
        check_vma=False,
    )
```

```python
import functools

import jax
import jax.numpy as jnp
from jax import lax
from jax.experimental import pallas as pl
from jax.experimental.pallas import tpu as pltpu
from jax.sharding import PartitionSpec as P

NX = 48
NU = 16
SEC = 8
COLS = SEC * NU
GX = 4
GZ = 8
F32 = jnp.float32
BF16 = jnp.bfloat16
Z_ORDER = (4, 3, 5, 2, 6, 1, 7)
ARRIVE = (1, 7, 2, 6, 3, 5, 4)
RELAYED = 0


def split(a):
    high = a.astype(BF16)
    return high, (a - high.astype(F32)).astype(BF16)


def dot(a, b):
    return lax.dot_general(a, b, (((1,), (0,)), ((), ())), preferred_element_type=F32)


def mm(a, b):
    ah, al = split(a)
    bh, bl = split(b)
    return dot(ah, bh) + (dot(ah, bl) + dot(al, bh))


def sq(a):
    return a[:, :NX]


def transposed(a):
    return jnp.transpose(jnp.concatenate([a, jnp.zeros((128 - a.shape[0], 128), F32)], axis=0))


def body(
    a_hbm, b_hbm, q_hbm, r_hbm, d_hbm, t_hbm, i_hbm,
    h_ref, grad_ref,
    a_v, b_v, q_v, r_v, d_v, t_v, i_v,
    y_v, qy_v, x_tc, x_lr, z_tc, z_l, z_r, coef_a, coef_b, rhs,
    in_sem, xt_s, xt_r, xl_s, xl_r, zt_s, zt_r, zl_s, zl_r, zr_s, zr_r, w_s, w_r,
):
    me = lax.axis_index("horizon")
    z, x = me // GX, me % GX

    loads = [
        pltpu.make_async_copy(src.at[0], dst, in_sem.at[k])
        for k, (src, dst) in enumerate(
            ((a_hbm, a_v), (b_hbm, b_v), (d_hbm, d_v), (t_hbm, t_v), (q_hbm, q_v), (r_hbm, r_v))
        )
    ]
    loads.append(pltpu.make_async_copy(i_hbm, i_v, in_sem.at[6]))
    for load in loads:
        load.start()

    for g in range(GZ):
        z_r[g] = jnp.zeros((NX, COLS), F32)

    def x_peer(d):
        return z * GX + (x + d) % GX

    def z_peer(d):
        return ((z + d) % GZ) * GX + x

    barrier = pltpu.get_barrier_semaphore()
    for d in range(1, GX):
        pl.semaphore_signal(barrier, inc=1, device_id={"horizon": x_peer(d)}, device_id_type=pl.DeviceIdType.MESH)
    for d in range(1, GZ):
        pl.semaphore_signal(barrier, inc=1, device_id={"horizon": z_peer(d)}, device_id_type=pl.DeviceIdType.MESH)

    def remote(ref, send, recv, peer):
        return pltpu.make_async_remote_copy(
            src_ref=ref, dst_ref=ref, send_sem=send, recv_sem=recv,
            device_id={"horizon": peer}, device_id_type=pl.DeviceIdType.MESH,
        )

    for load in loads:
        load.wait()

    lane = lax.broadcasted_iota(jnp.int32, (NX, 128), 1)
    row = lax.broadcasted_iota(jnp.int32, (NX, 128), 0)
    unit = jnp.where(lane == row, 1.0, 0.0).astype(F32)

    vectors = jnp.concatenate(
        [
            jnp.concatenate([d_v[...], t_v[...], jnp.broadcast_to(i_v[...], (8, NX))], axis=0),
            jnp.zeros((24, 128 - NX), F32),
        ],
        axis=1,
    )
    columns = transposed(vectors)[:NX]
    init_row = vectors[2 * SEC : 2 * SEC + 1]

    def vector_at(k):
        return jnp.where(lane == NX, pltpu.roll(columns, (NX - k) % 128, 1), 0.0)

    wide = jnp.zeros((NX, 128 - NX), F32)
    controls = jnp.transpose(
        jnp.concatenate([b_v[...].reshape(COLS, NX), jnp.zeros((COLS, 128 - NX), F32)], axis=1)
    )[:NX]
    state = None
    for t in range(SEC):
        entry = vector_at(t)
        placed = jnp.where(lane // NU == t, controls, 0.0)
        added = jnp.concatenate([entry, placed], axis=1)
        if t == 0:
            state = added + jnp.concatenate([a_v[0], wide, jnp.zeros((NX, 128), F32)], axis=1)
        else:
            state = mm(a_v[t], state) + added
        error = jnp.concatenate([state[:, :128] - vector_at(SEC + t), state[:, 128:]], axis=1)
        y_v[NX * t : NX * (t + 1), :] = error
        qy_v[NX * t : NX * (t + 1), :] = mm(q_v[t], error)
    gram = mm(jnp.transpose(y_v[...]), qy_v[...])
    own_l = state[:, 128:]
    own_r = gram[:NX, 128:]
    own_t = sq(state)
    x_tc[x] = state[:, :128] + pltpu.roll(gram[:NX, :128], 64, 1)
    x_lr[x, 0] = own_l
    x_lr[x, 1] = own_r

    pl.semaphore_wait(barrier, GX - 1 + GZ - 1)
    sends = []

    def send(ref, s, r, peer):
        copy = remote(ref, s, r, peer)
        copy.start()
        sends.append(copy)

    for d in (2, 1, 3):
        send(x_tc.at[x], xt_s.at[d], xt_r.at[x], x_peer(d))
    for d in (2, 1, 3):
        send(x_lr.at[x], xl_s.at[d], xl_r.at[x], x_peer(d))

    for d in range(1, GX):
        i = (x + d) % GX
        remote(x_tc.at[i], xt_s.at[d], xt_r.at[i], x_peer(d)).wait_recv()

    def turned(packed):
        return transposed(packed)

    def mixed(packed, flip):
        return jnp.where(lane < NX, flip[:NX], jnp.where(lane < 64, 0.0, packed))

    def maps_of(packed):
        return jnp.where(lane < 64, packed, 0.0)

    def cost_of(packed):
        return jnp.where(lane < 64, pltpu.roll(packed, 64, 1), 0.0)

    def at_column(value):
        return jnp.where(lane == NX, value, 0.0)

    def choose(index, values):
        out = values[0]
        for k in range(1, len(values)):
            out = jnp.where(index == k, values[k], out)
        return out

    nothing = jnp.zeros((NX, 128), F32)

    xp = [x_tc[i] for i in range(GX)]
    xf = [turned(p) for p in xp]
    xm = [maps_of(p) for p in xp]
    backs = [unit, jnp.where(lane < NX, xf[0][:NX], 0.0)]
    gains = [cost_of(xp[0])]
    for i in range(1, GX):
        both = mm(sq(backs[i]), mixed(xp[i], xf[i]))
        backs.append(both)
        gains.append(cost_of(both))
    tails = [None] * GX
    after = [None] * GX
    tails[GX - 1], after[GX - 1] = nothing, unit
    tails[GX - 2], after[GX - 2] = gains[GX - 1], xm[GX - 1]
    for i in reversed(range(GX - 1)):
        stack = mm(sq(jnp.concatenate([tails[i], after[i]], axis=0)), xm[i])
        low = stack[:NX] + at_column(tails[i]) + gains[i]
        high = stack[NX:] + at_column(after[i])
        if i:
            tails[i - 1], after[i - 1] = low, high
    group_cost, group_map = low, high
    z_tc[z] = group_map + pltpu.roll(group_cost, 64, 1)
    for d in Z_ORDER:
        send(z_tc.at[z], zt_s.at[d], zt_r.at[z], z_peer(d))

    group_l = mm(sq(choose(x, after)), own_l)
    group_r = mm(sq(choose(x, backs[:GX])), own_r) + mm(sq(choose(x, tails)), own_l)
    z_l[z] = group_l
    z_r[z] = group_r
    for d in ARRIVE:
        send(z_l.at[z], zl_s.at[d], zl_r.at[z], z_peer(d))
    for d in ARRIVE:
        @pl.when((z + d) % GZ < z)
        def _():
            remote(z_r.at[z], zr_s.at[d], zr_r.at[z], z_peer(d)).start()

    for d in range(1, GZ):
        g = (z + d) % GZ
        remote(z_tc.at[g], zt_s.at[d], zt_r.at[g], z_peer(d)).wait_recv()

    zp = [z_tc[g] for g in range(GZ)]
    zf = [turned(p) for p in zp]
    zm = [maps_of(p) for p in zp]
    ups = [jnp.where(lane < NX, jnp.broadcast_to(init_row, (NX, 128)), 0.0)]
    gains = []
    for g in range(GZ):
        both = mm(sq(ups[g]), mixed(zp[g], zf[g]))
        gains.append(jnp.where(g > z, cost_of(both), 0.0))
        if g < GZ - 1:
            moved = both + jnp.where(g < z, zf[g][NX : NX + 1], 0.0)
            ups.append(jnp.where(lane < NX, jnp.where(g == z, unit, moved), 0.0))
    enter = at_column(jnp.sum(jnp.where(lane == row, choose(z, ups), 0.0), axis=1, keepdims=True))
    downs = [None] * GZ
    downs[GZ - 1] = nothing
    for g in reversed(range(1, GZ)):
        if g == GZ - 1:
            moved = gains[g]
        else:
            moved = mm(sq(downs[g]), zm[g]) + at_column(downs[g]) + gains[g]
        downs[g - 1] = jnp.where(g == z, unit, moved)
    for g in range(GZ):
        coef_a[g] = jnp.where(g > z, ups[g], nothing)
        coef_b[g] = downs[g]
    group_tail = choose(z, downs)

    def forward(k):
        g = (z + ARRIVE[k]) % GZ
        i = (x + 1) % GX
        remote(rhs.at[g, i], w_s.at[ARRIVE[k], 1], w_r.at[g, i], x_peer(1)).wait_recv()
        send(rhs.at[g, i], w_s.at[ARRIVE[k], 2], w_r.at[g, i], x_peer(3))

    for k, d in enumerate(ARRIVE):
        g = (z + d) % GZ
        remote(z_l.at[g], zl_s.at[d], zl_r.at[g], z_peer(d)).wait_recv()

        @pl.when(g > z)
        def _():
            remote(z_r.at[g], zr_s.at[d], zr_r.at[g], z_peer(d)).wait_recv()

        rhs[g, x] = mm(sq(coef_a[g]), z_r[g]) + mm(sq(coef_b[g]), z_l[g])
        if k >= RELAYED:
            send(rhs.at[g, x], w_s.at[d, 2], w_r.at[g, x], x_peer(2))
        for e in (3, 1):
            send(rhs.at[g, x], w_s.at[d, e], w_r.at[g, x], x_peer(e))
        if 2 <= k < RELAYED + 2:
            forward(k - 2)

    for d in range(1, GX):
        i = (x + d) % GX
        remote(x_lr.at[i], xl_s.at[d], xl_r.at[i], x_peer(d)).wait_recv()
    ups = [unit]
    gains = []
    for i in range(GX):
        both = mm(sq(ups[i]), mixed(xp[i], xf[i]))
        gains.append(jnp.where(i > x, cost_of(both), 0.0))
        ups.append(jnp.where(lane < NX, jnp.where(i > x, both, unit), 0.0))
    downs = [None] * GX
    downs[GX - 1] = mm(sq(ups[GX]), group_tail)
    for i in reversed(range(1, GX)):
        moved = mm(sq(downs[i]), xm[i]) + at_column(downs[i]) + gains[i]
        downs[i - 1] = jnp.where(i == x, unit, moved)
    own_tail = choose(x, downs)
    for i in range(GX):
        ca = jnp.where(i > x, ups[i], nothing)
        rhs[z, i] = mm(sq(ca), x_lr[i, 1]) + mm(sq(downs[i]), x_lr[i, 0])

    for i in range(GX - 1):
        enter = jnp.where(i < x, mm(sq(xm[i]), enter) + at_column(xm[i]), enter)
    leaving = mm(own_t, enter) + at_column(state[:, :128])
    costate = mm(sq(own_tail), leaving) + at_column(own_tail)
    grad_ref[...] = gram[NX : NX + 1, 128:] + jnp.sum(
        enter[:, NX : NX + 1] * own_r + costate[:, NX : NX + 1] * own_l, axis=0, keepdims=True
    )

    own_mt = choose(x, xf)[:NX]
    full_r = own_r + mm(sq(own_mt), mm(sq(own_tail), own_l))
    group_mt = choose(z, zf)[:NX]
    group_full = group_r + mm(sq(group_mt), mm(sq(group_tail), group_l))

    def factors(value):
        high, low = split(value)
        turned = jnp.transpose(
            jnp.concatenate([high.astype(F32), low.astype(F32), jnp.zeros((32, 128), F32)], axis=0)
        )
        return turned.astype(BF16)[:, : 2 * NX]

    def rows(left, right):
        high, low = split(right)
        return dot(left, jnp.concatenate([high, high], axis=0)) + dot(left[:, :NX], low)

    f_gl, f_gr = factors(group_l), factors(group_full)
    f_l, f_r = factors(own_l), factors(full_r)

    tile = gram[128:, 128:]
    cost = jnp.concatenate(
        [
            jnp.concatenate([r_v[t], jnp.zeros((NU, 128 - NU), F32)], axis=1)
            if t == 0
            else pltpu.roll(jnp.concatenate([r_v[t], jnp.zeros((NU, 128 - NU), F32)], axis=1), NU * t, 1)
            for t in range(SEC)
        ],
        axis=0,
    )
    for i in range(GX):
        left = jnp.where(i < x, f_r.astype(F32), f_l.astype(F32)).astype(BF16)
        block = rows(left, rhs[z, i])
        block = block + jnp.where(i == x, tile + cost, 0.0)
        h_ref[:, pl.ds(pl.multiple_of(z * (GX * COLS) + i * COLS, COLS), COLS)] = block

    for k, d in enumerate(ARRIVE):
        g = (z + d) % GZ
        left = jnp.where(g > z, f_gl.astype(F32), f_gr.astype(F32)).astype(BF16)
        for e in range(1, GX):
            i = (x + e) % GX
            if k >= RELAYED or e != 1:
                remote(rhs.at[g, i], w_s.at[d, e], w_r.at[g, i], x_peer(e)).wait_recv()
        right = jnp.concatenate([rhs[g, i] for i in range(GX)], axis=1)
        h_ref[:, pl.ds(pl.multiple_of(g * (GX * COLS), GX * COLS), GX * COLS)] = rows(left, right)

    for copy in sends:
        copy.wait_send()
    for d in Z_ORDER:
        @pl.when((z + d) % GZ < z)
        def _():
            remote(z_r.at[z], zr_s.at[d], zr_r.at[z], z_peer(d)).wait_send()


def condense(dynamics, inputs, state_cost, input_cost, drift, target, initial):
    dma = pltpu.SemaphoreType.DMA
    hessian, gradient = pl.pallas_call(
        body,
        out_shape=(
            jax.ShapeDtypeStruct((COLS, GX * GZ * COLS), F32),
            jax.ShapeDtypeStruct((1, COLS), F32),
        ),
        in_specs=[pl.BlockSpec(memory_space=pltpu.HBM)] * 7,
        out_specs=(
            pl.BlockSpec(memory_space=pltpu.VMEM),
            pl.BlockSpec(memory_space=pltpu.VMEM),
        ),
        scratch_shapes=[
            pltpu.VMEM((SEC, NX, NX), F32),
            pltpu.VMEM((SEC, NU, NX), F32),
            pltpu.VMEM((SEC, NX, NX), F32),
            pltpu.VMEM((SEC, NU, NU), F32),
            pltpu.VMEM((SEC, NX), F32),
            pltpu.VMEM((SEC, NX), F32),
            pltpu.VMEM((1, NX), F32),
            pltpu.VMEM((SEC * NX, 256), F32),
            pltpu.VMEM((SEC * NX, 256), F32),
            pltpu.VMEM((GX, NX, 128), F32),
            pltpu.VMEM((GX, 2, NX, COLS), F32),
            pltpu.VMEM((GZ, NX, 128), F32),
            pltpu.VMEM((GZ, NX, COLS), F32),
            pltpu.VMEM((GZ, NX, COLS), F32),
            pltpu.VMEM((GZ, NX, 128), F32),
            pltpu.VMEM((GZ, NX, 128), F32),
            pltpu.VMEM((GZ, GX, NX, COLS), F32),
            dma((7,)),
            dma((GX,)), dma((GX,)), dma((GX,)), dma((GX,)),
            dma((GZ,)), dma((GZ,)), dma((GZ,)), dma((GZ,)), dma((GZ,)), dma((GZ,)),
            dma((GZ, GX)), dma((GZ, GX)),
        ],
        compiler_params=pltpu.CompilerParams(
            collective_id=0, has_side_effects=True, vmem_limit_bytes=16 * 1024 * 1024
        ),
        name="condense",
    )(*(pltpu.with_memory_space_constraint(v, pltpu.HBM) for v in (dynamics, jnp.swapaxes(inputs, 2, 3), state_cost, input_cost, drift, target, initial)))
    return hessian[None], gradient


def solution(mesh):
    return jax.shard_map(
        condense,
        mesh=mesh,
        in_specs=(
            P("batch", "horizon", None, None),
            P("batch", "horizon", None, None),
            P("batch", "horizon", None, None),
            P("batch", "horizon", None, None),
            P("batch", "horizon", None),
            P("batch", "horizon", None),
            P("batch", None),
        ),
        out_specs=(P("batch", "horizon", None), P("batch", "horizon")),
        check_vma=False,
    )
```

```python
import functools

import jax
import jax.numpy as jnp
from jax import lax
from jax.experimental import pallas as pl
from jax.experimental.pallas import tpu as pltpu
from jax.sharding import PartitionSpec as P

NX = 48
NU = 16
SEC = 8
COLS = SEC * NU
GX = 4
GZ = 8
F32 = jnp.float32
BF16 = jnp.bfloat16
Z_ORDER = (4, 3, 5, 2, 6, 1, 7)
ARRIVE = (1, 7, 2, 6, 3, 5, 4)
HALF = NX // 2
HALVES = SEC // 2
NEAR = (1, 7, 2, 6)
FAR = (3, 5, 4)


def split(a):
    high = a.astype(BF16)
    return high, (a - high.astype(F32)).astype(BF16)


def dot(a, b):
    return lax.dot_general(a, b, (((1,), (0,)), ((), ())), preferred_element_type=F32)


def mm(a, b):
    ah, al = split(a)
    bh, bl = split(b)
    return dot(ah, bh) + (dot(ah, bl) + dot(al, bh))


def sq(a):
    return a[:, :NX]


def transposed(a):
    return jnp.transpose(jnp.concatenate([a, jnp.zeros((128 - a.shape[0], 128), F32)], axis=0))


def body(
    a_hbm, b_hbm, q_hbm, r_hbm, d_hbm, t_hbm, i_hbm,
    h_ref, grad_ref,
    a_v, b_v, q_v, r_v, d_v, t_v, i_v,
    y_v, qy_v, x_tc, x_lr, z_tc, z_f, z_l, z_r, coef_a, coef_b, rhs, fac,
    in_sem, xt_s, xt_r, xl_s, xl_r, zt_s, zt_r, zl_s, zl_r, zf_s, zf_r, zr_s, zr_r, w_s, w_r,
):
    me = lax.axis_index("horizon")
    z, x = me // GX, me % GX

    loads = [
        pltpu.make_async_copy(src.at[0], dst, in_sem.at[k])
        for k, (src, dst) in enumerate(
            ((a_hbm, a_v), (b_hbm, b_v), (d_hbm, d_v), (t_hbm, t_v), (q_hbm, q_v), (r_hbm, r_v))
        )
    ]
    loads.append(pltpu.make_async_copy(i_hbm, i_v, in_sem.at[6]))
    for load in loads:
        load.start()

    for g in range(GZ):
        z_r[g] = jnp.zeros((NX, COLS), F32)

    def x_peer(d):
        return z * GX + (x + d) % GX

    def z_peer(d):
        return ((z + d) % GZ) * GX + x

    barrier = pltpu.get_barrier_semaphore()
    for d in range(1, GX):
        pl.semaphore_signal(barrier, inc=1, device_id={"horizon": x_peer(d)}, device_id_type=pl.DeviceIdType.MESH)
    for d in range(1, GZ):
        pl.semaphore_signal(barrier, inc=1, device_id={"horizon": z_peer(d)}, device_id_type=pl.DeviceIdType.MESH)

    def remote(ref, send, recv, peer, into=None):
        return pltpu.make_async_remote_copy(
            src_ref=ref, dst_ref=ref if into is None else into, send_sem=send, recv_sem=recv,
            device_id={"horizon": peer}, device_id_type=pl.DeviceIdType.MESH,
        )

    for load in loads:
        load.wait()

    lane = lax.broadcasted_iota(jnp.int32, (NX, 128), 1)
    row = lax.broadcasted_iota(jnp.int32, (NX, 128), 0)
    unit = jnp.where(lane == row, 1.0, 0.0).astype(F32)

    vectors = jnp.concatenate(
        [
            jnp.concatenate([d_v[...], t_v[...], jnp.broadcast_to(i_v[...], (8, NX))], axis=0),
            jnp.zeros((24, 128 - NX), F32),
        ],
        axis=1,
    )
    columns = transposed(vectors)[:NX]
    init_row = vectors[2 * SEC : 2 * SEC + 1]

    def vector_at(k):
        return jnp.where(lane == NX, pltpu.roll(columns, (NX - k) % 128, 1), 0.0)

    wide = jnp.zeros((NX, 128 - NX), F32)
    controls = jnp.transpose(
        jnp.concatenate([b_v[...].reshape(COLS, NX), jnp.zeros((COLS, 128 - NX), F32)], axis=1)
    )[:NX]
    def added(t):
        return jnp.concatenate([vector_at(t), jnp.where(lane // NU == t, controls, 0.0)], axis=1)

    def first(t):
        return added(t) + jnp.concatenate([a_v[t], wide, jnp.zeros((NX, 128), F32)], axis=1)

    early, late = [first(0)], [first(HALVES)]
    for t in range(1, HALVES):
        early.append(mm(a_v[t], early[-1]) + added(t))
        late.append(mm(a_v[HALVES + t], late[-1]) + added(HALVES + t))
    joined = mm(jnp.concatenate([sq(v) for v in late], axis=0), early[-1])
    narrow = jnp.concatenate([lane, lane + 128], axis=1) < NX
    states = early + [
        joined[NX * t : NX * (t + 1)] + jnp.where(narrow, 0.0, late[t]) for t in range(HALVES)
    ]
    state = states[-1]
    for t in range(SEC):
        error = jnp.concatenate([states[t][:, :128] - vector_at(SEC + t), states[t][:, 128:]], axis=1)
        y_v[NX * t : NX * (t + 1), :] = error
        qy_v[NX * t : NX * (t + 1), :] = mm(q_v[t], error)
    gram = mm(jnp.transpose(y_v[...]), qy_v[...])
    own_l = state[:, 128:]
    own_r = gram[:NX, 128:]
    own_t = sq(state)
    x_tc[x] = state[:, :128] + pltpu.roll(gram[:NX, :128], 64, 1)
    x_lr[x, 0] = own_l
    x_lr[x, 1] = own_r

    pl.semaphore_wait(barrier, GX - 1 + GZ - 1)
    sends = []

    def send(ref, s, r, peer, into=None):
        copy = remote(ref, s, r, peer, into)
        copy.start()
        sends.append(copy)

    for d in (2, 1, 3):
        send(x_tc.at[x], xt_s.at[d], xt_r.at[x], x_peer(d))
    for d in Z_ORDER:
        send(x_lr.at[x, 0], zl_s.at[d], zl_r.at[z], z_peer(d), z_l.at[z])
    for d in (2, 1, 3):
        send(x_lr.at[x], xl_s.at[d], xl_r.at[x], x_peer(d))

    for d in range(1, GX):
        i = (x + d) % GX
        remote(x_tc.at[i], xt_s.at[d], xt_r.at[i], x_peer(d)).wait_recv()

    def turned(packed):
        return transposed(packed)

    def mixed(packed, flip):
        return jnp.where(lane < NX, flip[:NX], jnp.where(lane < 64, 0.0, packed))

    def maps_of(packed):
        return jnp.where(lane < 64, packed, 0.0)

    def cost_of(packed):
        return jnp.where(lane < 64, pltpu.roll(packed, 64, 1), 0.0)

    def at_column(value):
        return jnp.where(lane == NX, value, 0.0)

    def choose(index, values):
        out = values[0]
        for k in range(1, len(values)):
            out = jnp.where(index == k, values[k], out)
        return out

    nothing = jnp.zeros((NX, 128), F32)

    xp = [x_tc[i] for i in range(GX)]
    xf = [turned(p) for p in xp]
    xm = [maps_of(p) for p in xp]
    backs = [unit, jnp.where(lane < NX, xf[0][:NX], 0.0)]
    gains = [cost_of(xp[0])]
    for i in range(1, GX):
        both = mm(sq(backs[i]), mixed(xp[i], xf[i]))
        backs.append(both)
        gains.append(cost_of(both))
    tails = [None] * GX
    after = [None] * GX
    tails[GX - 1], after[GX - 1] = nothing, unit
    tails[GX - 2], after[GX - 2] = gains[GX - 1], xm[GX - 1]
    for i in reversed(range(GX - 1)):
        stack = mm(sq(jnp.concatenate([tails[i], after[i]], axis=0)), xm[i])
        low = stack[:NX] + at_column(tails[i]) + gains[i]
        high = stack[NX:] + at_column(after[i])
        if i:
            tails[i - 1], after[i - 1] = low, high
    group_cost, group_map = low, high
    z_tc[z] = group_map + pltpu.roll(group_cost, 64, 1)
    for d in Z_ORDER:
        send(z_tc.at[z], zt_s.at[d], zt_r.at[z], z_peer(d))

    follow = jnp.where(lane < NX, choose(x, after), 0.0)
    z_f[z] = follow[:HALF] + pltpu.roll(follow[HALF:], 64, 1)
    group_l = mm(sq(follow), own_l)
    group_r = mm(sq(choose(x, backs[:GX])), own_r) + mm(sq(choose(x, tails)), own_l)
    z_r[z] = group_r
    for d in ARRIVE:
        send(z_f.at[z], zf_s.at[d], zf_r.at[z], z_peer(d))

        @pl.when((z + d) % GZ < z)
        def _():
            remote(z_r.at[z], zr_s.at[d], zr_r.at[z], z_peer(d)).start()

    for d in range(1, GX):
        i = (x + d) % GX
        remote(x_lr.at[i], xl_s.at[d], xl_r.at[i], x_peer(d)).wait_recv()
    own_follow = choose(x, after)
    ups = [unit]
    gains = []
    for i in range(GX):
        both = mm(sq(ups[i]), mixed(xp[i], xf[i]))
        gains.append(jnp.where(i > x, cost_of(both), 0.0))
        ups.append(jnp.where(lane < NX, jnp.where(i > x, both, unit), 0.0))
    downs = [None] * GX
    downs[GX - 1] = nothing
    for i in reversed(range(1, GX)):
        moved = mm(sq(downs[i]), xm[i]) + at_column(downs[i]) + gains[i]
        downs[i - 1] = jnp.where(i == x, unit, moved)
    near_tail = choose(x, downs)
    to_exit = sq(ups[GX])
    base, carried = [], []
    for i in range(GX):
        ca = jnp.where(i > x, ups[i], nothing)
        base.append(mm(sq(ca), x_lr[i, 1]) + mm(sq(downs[i]), x_lr[i, 0]))
        carried.append(jnp.where(i >= x, mm(sq(after[i]), x_lr[i, 0]), 0.0))
    before = [unit, xm[0]]
    for i in range(1, GX):
        before.append(mm(sq(xm[i]), before[i]) + at_column(xm[i]))
    reach = jnp.concatenate([choose(x, before[:GX]), choose(x, before[1:])], axis=0)
    own_mt = choose(x, xf)[:NX]

    def factors(value):
        high, low = split(value)
        stacked = jnp.concatenate([high.astype(F32), low.astype(F32), jnp.zeros((32, 128), F32)], axis=0)
        return jnp.transpose(stacked).astype(BF16)

    fac[1] = factors(group_l)
    fac[3] = factors(own_l)

    for d in range(1, GZ):
        g = (z + d) % GZ
        remote(z_tc.at[g], zt_s.at[d], zt_r.at[g], z_peer(d)).wait_recv()

    zp = [z_tc[g] for g in range(GZ)]
    zf = [turned(p) for p in zp]
    zm = [maps_of(p) for p in zp]
    ups = [jnp.where(lane < NX, jnp.broadcast_to(init_row, (NX, 128)), 0.0)]
    gains = []
    for g in range(GZ):
        both = mm(sq(ups[g]), mixed(zp[g], zf[g]))
        gains.append(jnp.where(g > z, cost_of(both), 0.0))
        if g < GZ - 1:
            moved = both + jnp.where(g < z, zf[g][NX : NX + 1], 0.0)
            ups.append(jnp.where(lane < NX, jnp.where(g == z, unit, moved), 0.0))
    enter = at_column(jnp.sum(jnp.where(lane == row, choose(z, ups), 0.0), axis=1, keepdims=True))
    downs = [None] * GZ
    downs[GZ - 1] = nothing
    for g in reversed(range(1, GZ)):
        if g == GZ - 1:
            moved = gains[g]
        else:
            moved = mm(sq(downs[g]), zm[g]) + at_column(downs[g]) + gains[g]
        downs[g - 1] = jnp.where(g == z, unit, moved)
    for g in range(GZ):
        coef_a[g] = jnp.where(g > z, ups[g], nothing)
        coef_b[g] = downs[g]
    group_tail = choose(z, downs)

    def pieces(batch):
        through = {}
        for d in batch:
            g = (z + d) % GZ
            remote(z_l.at[g], zl_s.at[d], zl_r.at[g], z_peer(d)).wait_recv()
            remote(z_f.at[g], zf_s.at[d], zf_r.at[g], z_peer(d)).wait_recv()
            packed = z_f[g]
            through[d] = mm(
                sq(coef_b[g]), jnp.concatenate([packed, pltpu.roll(packed, 64, 1)], axis=0)
            )

            @pl.when(g > z)
            def _():
                remote(z_r.at[g], zr_s.at[d], zr_r.at[g], z_peer(d)).wait_recv()

        for d in batch:
            g = (z + d) % GZ
            rhs[g, x] = mm(sq(coef_a[g]), z_r[g]) + mm(sq(through[d]), z_l[g])
        for d in batch:
            g = (z + d) % GZ
            for e in (2, 3, 1):
                send(rhs.at[g, x], w_s.at[d, e], w_r.at[g, x], x_peer(e))

    for d in ARRIVE:
        pieces((d,))

    inner = mm(sq(group_tail), jnp.concatenate([own_follow] + carried, axis=1))
    inner = jnp.concatenate([inner[:, :128] + at_column(group_tail), inner[:, 128:]], axis=1)
    outer = mm(to_exit, inner)
    own_tail = near_tail + outer[:, :128]
    blocks = [base[i] + outer[:, 128 * (i + 1) : 128 * (i + 2)] for i in range(GX)]
    full_r = own_r + mm(sq(own_mt), choose(x, blocks))
    group_mt = choose(z, zf)[:NX]
    group_full = group_r + mm(
        sq(group_mt), choose(x, [inner[:, 128 * (i + 1) : 128 * (i + 2)] for i in range(GX)])
    )
    fac[0] = factors(group_full)
    fac[2] = factors(full_r)
    both = mm(sq(reach), enter) + jnp.where(
        jnp.concatenate([lane, lane], axis=0) == NX, reach, 0.0
    )
    costate = mm(sq(own_tail), both[NX:]) + at_column(own_tail)
    grad_ref[...] = gram[NX : NX + 1, 128:] + jnp.sum(
        both[:NX, NX : NX + 1] * own_r + costate[:, NX : NX + 1] * own_l, axis=0, keepdims=True
    )

    def rows(left, right):
        high, low = split(right)
        return dot(left[:, : 2 * NX], jnp.concatenate([high, high], axis=0)) + dot(left[:, :NX], low)

    tile = gram[128:, 128:]
    cost = jnp.concatenate(
        [
            jnp.concatenate([r_v[t], jnp.zeros((NU, 128 - NU), F32)], axis=1)
            if t == 0
            else pltpu.roll(jnp.concatenate([r_v[t], jnp.zeros((NU, 128 - NU), F32)], axis=1), NU * t, 1)
            for t in range(SEC)
        ],
        axis=0,
    )
    for i in range(GX):
        block = rows(fac[jnp.where(i < x, 2, 3)], blocks[i])
        block = block + jnp.where(i == x, tile + cost, 0.0)
        h_ref[:, pl.ds(pl.multiple_of(z * (GX * COLS) + i * COLS, COLS), COLS)] = block

    for batch in [(d,) for d in ARRIVE]:
        for d in batch:
            g = (z + d) % GZ
            for e in range(1, GX):
                i = (x + e) % GX
                remote(rhs.at[g, i], w_s.at[d, e], w_r.at[g, i], x_peer(e)).wait_recv()
        for d in batch:
            g = (z + d) % GZ
            right = jnp.concatenate([rhs[g, i] for i in range(GX)], axis=1)
            h_ref[:, pl.ds(pl.multiple_of(g * (GX * COLS), GX * COLS), GX * COLS)] = rows(
                fac[jnp.where(g > z, 1, 0)], right
            )

    for copy in sends:
        copy.wait_send()
    for d in Z_ORDER:
        @pl.when((z + d) % GZ < z)
        def _():
            remote(z_r.at[z], zr_s.at[d], zr_r.at[z], z_peer(d)).wait_send()


def condense(dynamics, inputs, state_cost, input_cost, drift, target, initial):
    dma = pltpu.SemaphoreType.DMA
    hessian, gradient = pl.pallas_call(
        body,
        out_shape=(
            jax.ShapeDtypeStruct((COLS, GX * GZ * COLS), F32),
            jax.ShapeDtypeStruct((1, COLS), F32),
        ),
        in_specs=[pl.BlockSpec(memory_space=pltpu.HBM)] * 7,
        out_specs=(
            pl.BlockSpec(memory_space=pltpu.VMEM),
            pl.BlockSpec(memory_space=pltpu.VMEM),
        ),
        scratch_shapes=[
            pltpu.VMEM((SEC, NX, NX), F32),
            pltpu.VMEM((SEC, NU, NX), F32),
            pltpu.VMEM((SEC, NX, NX), F32),
            pltpu.VMEM((SEC, NU, NU), F32),
            pltpu.VMEM((SEC, NX), F32),
            pltpu.VMEM((SEC, NX), F32),
            pltpu.VMEM((1, NX), F32),
            pltpu.VMEM((SEC * NX, 256), F32),
            pltpu.VMEM((SEC * NX, 256), F32),
            pltpu.VMEM((GX, NX, 128), F32),
            pltpu.VMEM((GX, 2, NX, COLS), F32),
            pltpu.VMEM((GZ, NX, 128), F32),
            pltpu.VMEM((GZ, HALF, 128), F32),
            pltpu.VMEM((GZ, NX, COLS), F32),
            pltpu.VMEM((GZ, NX, COLS), F32),
            pltpu.VMEM((GZ, NX, 128), F32),
            pltpu.VMEM((GZ, NX, 128), F32),
            pltpu.VMEM((GZ, GX, NX, COLS), F32),
            pltpu.VMEM((4, 128, 128), BF16),
            dma((7,)),
            dma((GX,)), dma((GX,)), dma((GX,)), dma((GX,)),
            dma((GZ,)), dma((GZ,)), dma((GZ,)), dma((GZ,)), dma((GZ,)), dma((GZ,)), dma((GZ,)), dma((GZ,)),
            dma((GZ, GX)), dma((GZ, GX)),
        ],
        compiler_params=pltpu.CompilerParams(
            collective_id=0, has_side_effects=True, vmem_limit_bytes=16 * 1024 * 1024
        ),
        name="condense",
    )(*(pltpu.with_memory_space_constraint(v, pltpu.HBM) for v in (dynamics, jnp.swapaxes(inputs, 2, 3), state_cost, input_cost, drift, target, initial)))
    return hessian[None], gradient


def solution(mesh):
    return jax.shard_map(
        condense,
        mesh=mesh,
        in_specs=(
            P("batch", "horizon", None, None),
            P("batch", "horizon", None, None),
            P("batch", "horizon", None, None),
            P("batch", "horizon", None, None),
            P("batch", "horizon", None),
            P("batch", "horizon", None),
            P("batch", None),
        ),
        out_specs=(P("batch", "horizon", None), P("batch", "horizon")),
        check_vma=False,
    )
```

```python
import functools

import jax
import jax.numpy as jnp
from jax import lax
from jax.experimental import pallas as pl
from jax.experimental.pallas import tpu as pltpu
from jax.sharding import PartitionSpec as P

NX = 48
NU = 16
SEC = 8
COLS = SEC * NU
GX = 4
GZ = 8
F32 = jnp.float32
BF16 = jnp.bfloat16
Z_ORDER = (4, 3, 5, 2, 6, 1, 7)
ARRIVE = (1, 7, 2, 6, 3, 5, 4)
HALF = NX // 2
HALVES = SEC // 2
SPLITS = 4
NEAR = (1, 7, 2, 6)
FAR = (3, 5, 4)


def split(a):
    high = a.astype(BF16)
    return high, (a - high.astype(F32)).astype(BF16)


def dot(a, b):
    return lax.dot_general(a, b, (((1,), (0,)), ((), ())), preferred_element_type=F32)


def mm(a, b):
    ah, al = split(a)
    bh, bl = split(b)
    n = a.shape[0]
    both = dot(jnp.concatenate([ah, al], axis=0), bh)
    return both[:n] + (dot(ah, bl) + both[n:])


def sq(a):
    return a[:, :NX]


def transposed(a):
    return jnp.transpose(jnp.concatenate([a, jnp.zeros((128 - a.shape[0], 128), F32)], axis=0))


def body(
    a_hbm, b_hbm, q_hbm, r_hbm, d_hbm, t_hbm, i_hbm,
    h_ref, grad_ref,
    a_v, b_v, q_v, r_v, d_v, t_v, i_v,
    y_v, qy_v, x_tc, x_lr, z_tc, z_f, z_l, z_r, coef_a, coef_b, rhs, fac,
    in_sem, xt_s, xt_r, xl_s, xl_r, zt_s, zt_r, zl_s, zl_r, zf_s, zf_r, zr_s, zr_r, w_s, w_r,
):
    me = lax.axis_index("horizon")
    z, x = me // GX, me % GX

    loads = [
        pltpu.make_async_copy(src.at[0], dst, in_sem.at[k])
        for k, (src, dst) in enumerate(
            ((a_hbm, a_v), (b_hbm, b_v), (d_hbm, d_v), (t_hbm, t_v), (q_hbm, q_v), (r_hbm, r_v))
        )
    ]
    loads.append(pltpu.make_async_copy(i_hbm, i_v, in_sem.at[6]))
    for load in loads:
        load.start()

    for g in range(GZ):
        z_r[g] = jnp.zeros((NX, COLS), F32)

    def x_peer(d):
        return z * GX + (x + d) % GX

    def z_peer(d):
        return ((z + d) % GZ) * GX + x

    barrier = pltpu.get_barrier_semaphore()
    for d in range(1, GX):
        pl.semaphore_signal(barrier, inc=1, device_id={"horizon": x_peer(d)}, device_id_type=pl.DeviceIdType.MESH)
    for d in range(1, GZ):
        pl.semaphore_signal(barrier, inc=1, device_id={"horizon": z_peer(d)}, device_id_type=pl.DeviceIdType.MESH)

    def remote(ref, send, recv, peer, into=None):
        return pltpu.make_async_remote_copy(
            src_ref=ref, dst_ref=ref if into is None else into, send_sem=send, recv_sem=recv,
            device_id={"horizon": peer}, device_id_type=pl.DeviceIdType.MESH,
        )

    for k in (0, 1, 2, 3, 6):
        loads[k].wait()

    lane = lax.broadcasted_iota(jnp.int32, (NX, 128), 1)
    row = lax.broadcasted_iota(jnp.int32, (NX, 128), 0)
    unit = jnp.where(lane == row, 1.0, 0.0).astype(F32)

    vectors = jnp.concatenate(
        [
            jnp.concatenate([d_v[...], t_v[...], jnp.broadcast_to(i_v[...], (8, NX))], axis=0),
            jnp.zeros((24, 128 - NX), F32),
        ],
        axis=1,
    )
    columns = transposed(vectors)[:NX]
    init_row = vectors[2 * SEC : 2 * SEC + 1]

    def vector_at(k):
        return jnp.where(lane == NX, pltpu.roll(columns, (NX - k) % 128, 1), 0.0)

    wide = jnp.zeros((NX, 128 - NX), F32)
    controls = jnp.transpose(
        jnp.concatenate([b_v[...].reshape(COLS, NX), jnp.zeros((COLS, 128 - NX), F32)], axis=1)
    )[:NX]
    def added(t):
        return jnp.concatenate([vector_at(t), jnp.where(lane // NU == t, controls, 0.0)], axis=1)

    def first(t):
        return added(t) + jnp.concatenate([a_v[t], wide, jnp.zeros((NX, 128), F32)], axis=1)

    early, late = [first(0)], [first(HALVES)]
    for t in range(1, HALVES):
        early.append(mm(a_v[t], early[-1]) + added(t))
        late.append(mm(a_v[HALVES + t], late[-1]) + added(HALVES + t))
    joined = mm(jnp.concatenate([sq(v) for v in late], axis=0), early[-1])
    narrow = jnp.concatenate([lane, lane + 128], axis=1) < NX
    states = early + [
        joined[NX * t : NX * (t + 1)] + jnp.where(narrow, 0.0, late[t]) for t in range(HALVES)
    ]
    state = states[-1]
    loads[4].wait()
    for t in range(SEC):
        error = jnp.concatenate([states[t][:, :128] - vector_at(SEC + t), states[t][:, 128:]], axis=1)
        y_v[NX * t : NX * (t + 1), :] = error
        qy_v[NX * t : NX * (t + 1), :] = mm(q_v[t], error)
    gram = mm(jnp.transpose(y_v[...]), qy_v[...])
    own_l = state[:, 128:]
    own_r = gram[:NX, 128:]
    own_t = sq(state)
    x_tc[x] = state[:, :128] + pltpu.roll(gram[:NX, :128], 64, 1)
    x_lr[x, 0] = own_l
    x_lr[x, 1] = own_r

    pl.semaphore_wait(barrier, GX - 1 + GZ - 1)
    sends = []

    def send(ref, s, r, peer, into=None):
        copy = remote(ref, s, r, peer, into)
        copy.start()
        sends.append(copy)

    for d in (2, 1, 3):
        send(x_tc.at[x], xt_s.at[d], xt_r.at[x], x_peer(d))
    for d in Z_ORDER:
        send(x_lr.at[x, 0], zl_s.at[d], zl_r.at[z], z_peer(d), z_l.at[z])
    for d in (2, 1, 3):
        send(x_lr.at[x], xl_s.at[d], xl_r.at[x], x_peer(d))

    for d in range(1, GX):
        i = (x + d) % GX
        remote(x_tc.at[i], xt_s.at[d], xt_r.at[i], x_peer(d)).wait_recv()

    def turned(packed):
        return transposed(packed)

    def mixed(packed, flip):
        return jnp.where(lane < NX, flip[:NX], jnp.where(lane < 64, 0.0, packed))

    def maps_of(packed):
        return jnp.where(lane < 64, packed, 0.0)

    def cost_of(packed):
        return jnp.where(lane < 64, pltpu.roll(packed, 64, 1), 0.0)

    def at_column(value):
        return jnp.where(lane == NX, value, 0.0)

    def choose(index, values):
        out = values[0]
        for k in range(1, len(values)):
            out = jnp.where(index == k, values[k], out)
        return out

    nothing = jnp.zeros((NX, 128), F32)

    xp = [x_tc[i] for i in range(GX)]
    xf = [turned(p) for p in xp]
    xm = [maps_of(p) for p in xp]
    first_back = jnp.where(lane < NX, xf[0][:NX], 0.0)
    one = mm(sq(first_back), mixed(xp[1], xf[1]))
    three = mm(xf[2][:NX, :NX], mixed(xp[3], xf[3]))
    gain_one, gain_three = cost_of(one), cost_of(three)
    low_cost = cost_of(xp[0]) + mm(sq(gain_one), xm[0]) + at_column(gain_one)
    high_cost = cost_of(xp[2]) + mm(sq(gain_three), xm[2]) + at_column(gain_three)
    low_map = mm(sq(xm[1]), xm[0]) + at_column(xm[1])
    high_map = mm(sq(xm[3]), xm[2]) + at_column(xm[3])
    low_back = jnp.where(lane < NX, one, 0.0)
    gain_high = mm(sq(low_back), high_cost)
    group_cost = low_cost + mm(sq(gain_high), low_map) + at_column(gain_high)
    group_map = mm(sq(high_map), low_map) + at_column(high_map)
    z_tc[z] = group_map + pltpu.roll(group_cost, 64, 1)
    for d in Z_ORDER:
        send(z_tc.at[z], zt_s.at[d], zt_r.at[z], z_peer(d))

    after = [mm(sq(high_map), xm[1]) + at_column(high_map), high_map, xm[3], unit]
    follow = jnp.where(lane < NX, choose(x, after), 0.0)
    z_f[z] = follow[:HALF] + pltpu.roll(follow[HALF:], 64, 1)
    backs = [unit, first_back, low_back, mm(sq(low_back), xf[2][:NX])]
    tails = [gain_one + mm(sq(gain_high), xm[1]), gain_high, mm(sq(backs[3]), cost_of(xp[3])), nothing]
    group_l = mm(sq(follow), own_l)
    group_r = mm(sq(choose(x, backs)), own_r) + mm(sq(choose(x, tails)), own_l)
    z_r[z] = group_r
    for d in ARRIVE:
        send(z_f.at[z], zf_s.at[d], zf_r.at[z], z_peer(d))

        @pl.when((z + d) % GZ < z)
        def _():
            remote(z_r.at[z], zr_s.at[d], zr_r.at[z], z_peer(d)).start()

    for d in range(1, GX):
        i = (x + d) % GX
        remote(x_lr.at[i], xl_s.at[d], xl_r.at[i], x_peer(d)).wait_recv()
    own_follow = choose(x, after)
    ups = [unit]
    gains = []
    for i in range(GX):
        both = mm(sq(ups[i]), mixed(xp[i], xf[i]))
        gains.append(jnp.where(i > x, cost_of(both), 0.0))
        ups.append(jnp.where(lane < NX, jnp.where(i > x, both, unit), 0.0))
    downs = [None] * GX
    downs[GX - 1] = nothing
    for i in reversed(range(1, GX)):
        moved = mm(sq(downs[i]), xm[i]) + at_column(downs[i]) + gains[i]
        downs[i - 1] = jnp.where(i == x, unit, moved)
    near_tail = choose(x, downs)
    to_exit = sq(ups[GX])
    base, carried = [], []
    for i in range(GX):
        ca = jnp.where(i > x, ups[i], nothing)
        base.append(mm(sq(ca), x_lr[i, 1]) + mm(sq(downs[i]), x_lr[i, 0]))
        carried.append(jnp.where(i >= x, mm(sq(after[i]), x_lr[i, 0]), 0.0))
    before = [unit, xm[0], low_map, mm(sq(xm[2]), low_map) + at_column(xm[2]), group_map]
    reach = jnp.concatenate([choose(x, before[:GX]), choose(x, before[1:])], axis=0)
    own_mt = choose(x, xf)[:NX]

    def factors(value):
        high, low = split(value)
        stacked = jnp.concatenate([high.astype(F32), low.astype(F32), jnp.zeros((32, 128), F32)], axis=0)
        return jnp.transpose(stacked).astype(BF16)

    fac[1] = factors(group_l)
    fac[3] = factors(own_l)

    for d in range(1, GZ):
        g = (z + d) % GZ
        remote(z_tc.at[g], zt_s.at[d], zt_r.at[g], z_peer(d)).wait_recv()

    zp = [z_tc[g] for g in range(GZ)]
    zf = [turned(p) for p in zp]
    zm = [maps_of(p) for p in zp]
    ups = [jnp.where(lane < NX, jnp.broadcast_to(init_row, (NX, 128)), 0.0)]
    gains = []
    for g in range(GZ):
        both = mm(sq(ups[g]), mixed(zp[g], zf[g]))
        gains.append(jnp.where(g > z, cost_of(both), 0.0))
        if g < GZ - 1:
            moved = both + jnp.where(g < z, zf[g][NX : NX + 1], 0.0)
            ups.append(jnp.where(lane < NX, jnp.where(g == z, unit, moved), 0.0))
    enter = at_column(jnp.sum(jnp.where(lane == row, choose(z, ups), 0.0), axis=1, keepdims=True))
    downs = [None] * GZ
    downs[GZ - 1] = nothing
    for g in reversed(range(1, GZ)):
        if g == GZ - 1:
            moved = gains[g]
        else:
            moved = mm(sq(downs[g]), zm[g]) + at_column(downs[g]) + gains[g]
        downs[g - 1] = jnp.where(g == z, unit, moved)
    for g in range(GZ):
        coef_a[g] = jnp.where(g > z, ups[g], nothing)
        coef_b[g] = downs[g]
    group_tail = choose(z, downs)

    def pieces(batch):
        through = {}
        for d in batch:
            g = (z + d) % GZ
            remote(z_l.at[g], zl_s.at[d], zl_r.at[g], z_peer(d)).wait_recv()
            remote(z_f.at[g], zf_s.at[d], zf_r.at[g], z_peer(d)).wait_recv()
            packed = z_f[g]
            through[d] = mm(
                sq(coef_b[g]), jnp.concatenate([packed, pltpu.roll(packed, 64, 1)], axis=0)
            )

            @pl.when(g > z)
            def _():
                remote(z_r.at[g], zr_s.at[d], zr_r.at[g], z_peer(d)).wait_recv()

        for d in batch:
            g = (z + d) % GZ
            rhs[g, x] = mm(sq(coef_a[g]), z_r[g]) + mm(sq(through[d]), z_l[g])
        for d in batch:
            g = (z + d) % GZ
            for e in (2, 3, 1):
                send(rhs.at[g, x], w_s.at[d, e], w_r.at[g, x], x_peer(e))

    for d in ARRIVE:
        pieces((d,))

    inner = mm(sq(group_tail), jnp.concatenate([own_follow] + carried, axis=1))
    inner = jnp.concatenate([inner[:, :128] + at_column(group_tail), inner[:, 128:]], axis=1)
    outer = mm(to_exit, inner)
    own_tail = near_tail + outer[:, :128]
    blocks = [base[i] + outer[:, 128 * (i + 1) : 128 * (i + 2)] for i in range(GX)]
    full_r = own_r + mm(sq(own_mt), choose(x, blocks))
    group_mt = choose(z, zf)[:NX]
    group_full = group_r + mm(
        sq(group_mt), choose(x, [inner[:, 128 * (i + 1) : 128 * (i + 2)] for i in range(GX)])
    )
    fac[0] = factors(group_full)
    fac[2] = factors(full_r)
    both = mm(sq(reach), enter) + jnp.where(
        jnp.concatenate([lane, lane], axis=0) == NX, reach, 0.0
    )
    costate = mm(sq(own_tail), both[NX:]) + at_column(own_tail)
    grad_ref[...] = gram[NX : NX + 1, 128:] + jnp.sum(
        both[:NX, NX : NX + 1] * own_r + costate[:, NX : NX + 1] * own_l, axis=0, keepdims=True
    )

    def rows(left, right):
        high, low = split(right)
        return dot(left[:, : 2 * NX], jnp.concatenate([high, high], axis=0)) + dot(left[:, :NX], low)

    loads[5].wait()
    tile = gram[128:, 128:]
    cost = jnp.concatenate(
        [
            jnp.concatenate([r_v[t], jnp.zeros((NU, 128 - NU), F32)], axis=1)
            if t == 0
            else pltpu.roll(jnp.concatenate([r_v[t], jnp.zeros((NU, 128 - NU), F32)], axis=1), NU * t, 1)
            for t in range(SEC)
        ],
        axis=0,
    )
    for i in range(GX):
        block = rows(fac[jnp.where(i < x, 2, 3)], blocks[i])
        block = block + jnp.where(i == x, tile + cost, 0.0)
        h_ref[:, pl.ds(pl.multiple_of(z * (GX * COLS) + i * COLS, COLS), COLS)] = block

    for batch in [(d,) for d in ARRIVE]:
        for d in batch:
            g = (z + d) % GZ
            for e in range(1, GX):
                i = (x + e) % GX
                remote(rhs.at[g, i], w_s.at[d, e], w_r.at[g, i], x_peer(e)).wait_recv()
        for d in batch:
            g = (z + d) % GZ
            right = jnp.concatenate([rhs[g, i] for i in range(GX)], axis=1)
            h_ref[:, pl.ds(pl.multiple_of(g * (GX * COLS), GX * COLS), GX * COLS)] = rows(
                fac[jnp.where(g > z, 1, 0)], right
            )

    for copy in sends:
        copy.wait_send()
    for d in Z_ORDER:
        @pl.when((z + d) % GZ < z)
        def _():
            remote(z_r.at[z], zr_s.at[d], zr_r.at[z], z_peer(d)).wait_send()


def settle(h_v, g_v, h_out, g_out, sem):
    size = COLS // SPLITS
    copies = [pltpu.make_async_copy(g_v, g_out, sem.at[SPLITS])]
    for k in range(SPLITS):
        part = pl.ds(size * k, size)
        copies.append(pltpu.make_async_copy(h_v.at[part], h_out.at[0, part], sem.at[k]))
    for copy in copies:
        copy.start()
    for copy in copies:
        copy.wait()


def condense(dynamics, inputs, state_cost, input_cost, drift, target, initial):
    dma = pltpu.SemaphoreType.DMA
    hessian, gradient = pl.pallas_call(
        body,
        out_shape=(
            jax.ShapeDtypeStruct((COLS, GX * GZ * COLS), F32),
            jax.ShapeDtypeStruct((1, COLS), F32),
        ),
        in_specs=[pl.BlockSpec(memory_space=pltpu.HBM)] * 7,
        out_specs=(
            pl.BlockSpec(memory_space=pltpu.VMEM),
            pl.BlockSpec(memory_space=pltpu.VMEM),
        ),
        scratch_shapes=[
            pltpu.VMEM((SEC, NX, NX), F32),
            pltpu.VMEM((SEC, NU, NX), F32),
            pltpu.VMEM((SEC, NX, NX), F32),
            pltpu.VMEM((SEC, NU, NU), F32),
            pltpu.VMEM((SEC, NX), F32),
            pltpu.VMEM((SEC, NX), F32),
            pltpu.VMEM((1, NX), F32),
            pltpu.VMEM((SEC * NX, 256), F32),
            pltpu.VMEM((SEC * NX, 256), F32),
            pltpu.VMEM((GX, NX, 128), F32),
            pltpu.VMEM((GX, 2, NX, COLS), F32),
            pltpu.VMEM((GZ, NX, 128), F32),
            pltpu.VMEM((GZ, HALF, 128), F32),
            pltpu.VMEM((GZ, NX, COLS), F32),
            pltpu.VMEM((GZ, NX, COLS), F32),
            pltpu.VMEM((GZ, NX, 128), F32),
            pltpu.VMEM((GZ, NX, 128), F32),
            pltpu.VMEM((GZ, GX, NX, COLS), F32),
            pltpu.VMEM((4, 128, 128), BF16),
            dma((7,)),
            dma((GX,)), dma((GX,)), dma((GX,)), dma((GX,)),
            dma((GZ,)), dma((GZ,)), dma((GZ,)), dma((GZ,)), dma((GZ,)), dma((GZ,)), dma((GZ,)), dma((GZ,)),
            dma((GZ, GX)), dma((GZ, GX)),
        ],
        compiler_params=pltpu.CompilerParams(
            collective_id=0, has_side_effects=True, vmem_limit_bytes=16 * 1024 * 1024
        ),
        name="condense",
    )(*(pltpu.with_memory_space_constraint(v, pltpu.HBM) for v in (dynamics, jnp.swapaxes(inputs, 2, 3), state_cost, input_cost, drift, target, initial)))
    return pl.pallas_call(
        settle,
        out_shape=(
            jax.ShapeDtypeStruct((1, COLS, GX * GZ * COLS), F32),
            jax.ShapeDtypeStruct((1, COLS), F32),
        ),
        in_specs=[pl.BlockSpec(memory_space=pltpu.VMEM)] * 2,
        out_specs=(pl.BlockSpec(memory_space=pltpu.HBM), pl.BlockSpec(memory_space=pltpu.HBM)),
        scratch_shapes=[dma((SPLITS + 1,))],
        compiler_params=pltpu.CompilerParams(vmem_limit_bytes=4 * 1024 * 1024),
        name="settle",
    )(hessian, gradient)


def solution(mesh):
    return jax.shard_map(
        condense,
        mesh=mesh,
        in_specs=(
            P("batch", "horizon", None, None),
            P("batch", "horizon", None, None),
            P("batch", "horizon", None, None),
            P("batch", "horizon", None, None),
            P("batch", "horizon", None),
            P("batch", "horizon", None),
            P("batch", None),
        ),
        out_specs=(P("batch", "horizon", None), P("batch", "horizon")),
        check_vma=False,
    )
```

```python
import functools

import jax
import jax.numpy as jnp
from jax import lax
from jax.experimental import pallas as pl
from jax.experimental.pallas import tpu as pltpu
from jax.sharding import PartitionSpec as P

NX = 48
NU = 16
SEC = 8
COLS = SEC * NU
GX = 4
GZ = 8
F32 = jnp.float32
BF16 = jnp.bfloat16
Z_ORDER = (4, 3, 5, 2, 6, 1, 7)
ARRIVE = (1, 7, 2, 6, 5, 3, 4)
SENDS = (7, 1, 6, 2, 3, 5, 4)
HALF = NX // 2
HALVES = SEC // 2
NEAR = (1, 7, 2, 6)
FAR = (3, 5, 4)


def split(a):
    high = a.astype(BF16)
    return high, (a - high.astype(F32)).astype(BF16)


def dot(a, b):
    return lax.dot_general(a, b, (((1,), (0,)), ((), ())), preferred_element_type=F32)


def mm(a, b):
    ah, al = split(a)
    bh, bl = split(b)
    n = a.shape[0]
    both = dot(jnp.concatenate([ah, al], axis=0), bh)
    return both[:n] + (dot(ah, bl) + both[n:])


def rows(left, right):
    high, low = split(right)
    return dot(left[:, : 2 * NX], jnp.concatenate([high, high], axis=0)) + dot(left[:, :NX], low)


def sq(a):
    return a[:, :NX]


def transposed(a):
    return jnp.transpose(jnp.concatenate([a, jnp.zeros((128 - a.shape[0], 128), F32)], axis=0))


def body(
    a_hbm, b_hbm, q_hbm, r_hbm, d_hbm, t_hbm, i_hbm,
    h_ref, grad_ref, right_ref, left_ref,
    a_v, b_v, q_v, r_v, d_v, t_v, i_v,
    y_v, qy_v, x_tc, x_lr, z_tc, z_f, z_l, z_r, coef_a, coef_b, rhs, fac,
    in_sem, xt_s, xt_r, xl_s, xl_r, zt_s, zt_r, zl_s, zl_r, zf_s, zf_r, zr_s, zr_r, w_s, w_r,
):
    me = lax.axis_index("horizon")
    z, x = me // GX, me % GX

    loads = [
        pltpu.make_async_copy(src.at[0], dst, in_sem.at[k])
        for k, (src, dst) in enumerate(
            ((a_hbm, a_v), (b_hbm, b_v), (d_hbm, d_v), (t_hbm, t_v), (q_hbm, q_v), (r_hbm, r_v))
        )
    ]
    loads.append(pltpu.make_async_copy(i_hbm, i_v, in_sem.at[6]))
    for load in loads:
        load.start()

    for g in range(GZ):
        z_r[g] = jnp.zeros((NX, COLS), F32)

    def x_peer(d):
        return z * GX + (x + d) % GX

    def z_peer(d):
        return ((z + d) % GZ) * GX + x

    barrier = pltpu.get_barrier_semaphore()
    for d in range(1, GX):
        pl.semaphore_signal(barrier, inc=1, device_id={"horizon": x_peer(d)}, device_id_type=pl.DeviceIdType.MESH)
    for d in range(1, GZ):
        pl.semaphore_signal(barrier, inc=1, device_id={"horizon": z_peer(d)}, device_id_type=pl.DeviceIdType.MESH)

    def remote(ref, send, recv, peer, into=None):
        return pltpu.make_async_remote_copy(
            src_ref=ref, dst_ref=ref if into is None else into, send_sem=send, recv_sem=recv,
            device_id={"horizon": peer}, device_id_type=pl.DeviceIdType.MESH,
        )

    for k in (0, 1, 2, 3, 6):
        loads[k].wait()

    lane = lax.broadcasted_iota(jnp.int32, (NX, 128), 1)
    row = lax.broadcasted_iota(jnp.int32, (NX, 128), 0)
    unit = jnp.where(lane == row, 1.0, 0.0).astype(F32)

    vectors = jnp.concatenate(
        [
            jnp.concatenate([d_v[...], t_v[...], jnp.broadcast_to(i_v[...], (8, NX))], axis=0),
            jnp.zeros((24, 128 - NX), F32),
        ],
        axis=1,
    )
    columns = transposed(vectors)[:NX]
    init_row = vectors[2 * SEC : 2 * SEC + 1]

    def vector_at(k):
        return jnp.where(lane == NX, pltpu.roll(columns, (NX - k) % 128, 1), 0.0)

    wide = jnp.zeros((NX, 128 - NX), F32)
    controls = jnp.transpose(
        jnp.concatenate([b_v[...].reshape(COLS, NX), jnp.zeros((COLS, 128 - NX), F32)], axis=1)
    )[:NX]
    def added(t):
        return jnp.concatenate([vector_at(t), jnp.where(lane // NU == t, controls, 0.0)], axis=1)

    def first(t):
        return added(t) + jnp.concatenate([a_v[t], wide, jnp.zeros((NX, 128), F32)], axis=1)

    early, late = [first(0)], [first(HALVES)]
    for t in range(1, HALVES):
        early.append(mm(a_v[t], early[-1]) + added(t))
        late.append(mm(a_v[HALVES + t], late[-1]) + added(HALVES + t))
    joined = mm(jnp.concatenate([sq(v) for v in late], axis=0), early[-1])
    narrow = jnp.concatenate([lane, lane + 128], axis=1) < NX
    states = early + [
        joined[NX * t : NX * (t + 1)] + jnp.where(narrow, 0.0, late[t]) for t in range(HALVES)
    ]
    state = states[-1]
    loads[4].wait()
    for t in range(SEC):
        error = jnp.concatenate([states[t][:, :128] - vector_at(SEC + t), states[t][:, 128:]], axis=1)
        y_v[NX * t : NX * (t + 1), :] = error
        qy_v[NX * t : NX * (t + 1), :] = mm(q_v[t], error)
    gram = mm(jnp.transpose(y_v[...]), qy_v[...])
    own_l = state[:, 128:]
    own_r = gram[:NX, 128:]
    own_t = sq(state)
    x_tc[x] = state[:, :128] + pltpu.roll(gram[:NX, :128], 64, 1)
    x_lr[x, 0] = own_l
    x_lr[x, 1] = own_r

    pl.semaphore_wait(barrier, GX - 1 + GZ - 1)
    sends = []

    def send(ref, s, r, peer, into=None):
        copy = remote(ref, s, r, peer, into)
        copy.start()
        sends.append(copy)

    for d in (2, 1, 3):
        send(x_tc.at[x], xt_s.at[d], xt_r.at[x], x_peer(d))
    for d in Z_ORDER:
        send(x_lr.at[x, 0], zl_s.at[d], zl_r.at[z], z_peer(d), z_l.at[z])
    for d in (2, 1, 3):
        send(x_lr.at[x], xl_s.at[d], xl_r.at[x], x_peer(d))

    for d in range(1, GX):
        i = (x + d) % GX
        remote(x_tc.at[i], xt_s.at[d], xt_r.at[i], x_peer(d)).wait_recv()

    def turned(packed):
        return transposed(packed)

    def mixed(packed, flip):
        return jnp.where(lane < NX, flip[:NX], jnp.where(lane < 64, 0.0, packed))

    def maps_of(packed):
        return jnp.where(lane < 64, packed, 0.0)

    def cost_of(packed):
        return jnp.where(lane < 64, pltpu.roll(packed, 64, 1), 0.0)

    def at_column(value):
        return jnp.where(lane == NX, value, 0.0)

    def choose(index, values):
        out = values[0]
        for k in range(1, len(values)):
            out = jnp.where(index == k, values[k], out)
        return out

    nothing = jnp.zeros((NX, 128), F32)

    xp = [x_tc[i] for i in range(GX)]
    xf = [turned(p) for p in xp]
    xm = [maps_of(p) for p in xp]
    first_back = jnp.where(lane < NX, xf[0][:NX], 0.0)
    one = mm(sq(first_back), mixed(xp[1], xf[1]))
    three = mm(xf[2][:NX, :NX], mixed(xp[3], xf[3]))
    gain_one, gain_three = cost_of(one), cost_of(three)
    low_cost = cost_of(xp[0]) + mm(sq(gain_one), xm[0]) + at_column(gain_one)
    high_cost = cost_of(xp[2]) + mm(sq(gain_three), xm[2]) + at_column(gain_three)
    low_map = mm(sq(xm[1]), xm[0]) + at_column(xm[1])
    high_map = mm(sq(xm[3]), xm[2]) + at_column(xm[3])
    low_back = jnp.where(lane < NX, one, 0.0)
    gain_high = mm(sq(low_back), high_cost)
    group_cost = low_cost + mm(sq(gain_high), low_map) + at_column(gain_high)
    group_map = mm(sq(high_map), low_map) + at_column(high_map)
    z_tc[z] = group_map + pltpu.roll(group_cost, 64, 1)
    for d in Z_ORDER:
        send(z_tc.at[z], zt_s.at[d], zt_r.at[z], z_peer(d))

    after = [mm(sq(high_map), xm[1]) + at_column(high_map), high_map, xm[3], unit]
    follow = jnp.where(lane < NX, choose(x, after), 0.0)
    z_f[z] = follow[:HALF] + pltpu.roll(follow[HALF:], 64, 1)
    backs = [unit, first_back, low_back, mm(sq(low_back), xf[2][:NX])]
    tails = [gain_one + mm(sq(gain_high), xm[1]), gain_high, mm(sq(backs[3]), cost_of(xp[3])), nothing]
    group_l = mm(sq(follow), own_l)
    group_r = mm(sq(choose(x, backs)), own_r) + mm(sq(choose(x, tails)), own_l)
    z_r[z] = group_r
    for d in SENDS:
        send(z_f.at[z], zf_s.at[d], zf_r.at[z], z_peer(d))

        @pl.when((z + d) % GZ < z)
        def _():
            remote(z_r.at[z], zr_s.at[d], zr_r.at[z], z_peer(d)).start()

    for d in range(1, GX):
        i = (x + d) % GX
        remote(x_lr.at[i], xl_s.at[d], xl_r.at[i], x_peer(d)).wait_recv()
    own_follow = choose(x, after)
    ups = [unit]
    gains = []
    for i in range(GX):
        both = mm(sq(ups[i]), mixed(xp[i], xf[i]))
        gains.append(jnp.where(i > x, cost_of(both), 0.0))
        ups.append(jnp.where(lane < NX, jnp.where(i > x, both, unit), 0.0))
    downs = [None] * GX
    downs[GX - 1] = nothing
    for i in reversed(range(1, GX)):
        moved = mm(sq(downs[i]), xm[i]) + at_column(downs[i]) + gains[i]
        downs[i - 1] = jnp.where(i == x, unit, moved)
    near_tail = choose(x, downs)
    to_exit = sq(ups[GX])
    base, carried = [], []
    for i in range(GX):
        ca = jnp.where(i > x, ups[i], nothing)
        base.append(mm(sq(ca), x_lr[i, 1]) + mm(sq(downs[i]), x_lr[i, 0]))
        carried.append(jnp.where(i >= x, mm(sq(after[i]), x_lr[i, 0]), 0.0))
    before = [unit, xm[0], low_map, mm(sq(xm[2]), low_map) + at_column(xm[2]), group_map]
    reach = jnp.concatenate([choose(x, before[:GX]), choose(x, before[1:])], axis=0)
    own_mt = choose(x, xf)[:NX]

    def factors(value):
        high, low = split(value)
        stacked = jnp.concatenate([high.astype(F32), low.astype(F32), jnp.zeros((32, 128), F32)], axis=0)
        return jnp.transpose(stacked).astype(BF16)

    fac[1] = factors(group_l)
    fac[3] = factors(own_l)

    for d in range(1, GZ):
        g = (z + d) % GZ
        remote(z_tc.at[g], zt_s.at[d], zt_r.at[g], z_peer(d)).wait_recv()

    zp = [z_tc[g] for g in range(GZ)]
    zf = [turned(p) for p in zp]
    zm = [maps_of(p) for p in zp]
    ups = [jnp.where(lane < NX, jnp.broadcast_to(init_row, (NX, 128)), 0.0)]
    gains = []
    for g in range(GZ):
        both = mm(sq(ups[g]), mixed(zp[g], zf[g]))
        gains.append(jnp.where(g > z, cost_of(both), 0.0))
        if g < GZ - 1:
            moved = both + jnp.where(g < z, zf[g][NX : NX + 1], 0.0)
            ups.append(jnp.where(lane < NX, jnp.where(g == z, unit, moved), 0.0))
    enter = at_column(jnp.sum(jnp.where(lane == row, choose(z, ups), 0.0), axis=1, keepdims=True))
    downs = [None] * GZ
    downs[GZ - 1] = nothing
    for g in reversed(range(1, GZ)):
        if g == GZ - 1:
            moved = gains[g]
        else:
            moved = mm(sq(downs[g]), zm[g]) + at_column(downs[g]) + gains[g]
        downs[g - 1] = jnp.where(g == z, unit, moved)
    for g in range(GZ):
        coef_a[g] = jnp.where(g > z, ups[g], nothing)
        coef_b[g] = downs[g]
    group_tail = choose(z, downs)

    def pieces(batch):
        through = {}
        for d in batch:
            g = (z + d) % GZ
            remote(z_l.at[g], zl_s.at[d], zl_r.at[g], z_peer(d)).wait_recv()
            remote(z_f.at[g], zf_s.at[d], zf_r.at[g], z_peer(d)).wait_recv()
            packed = z_f[g]
            through[d] = mm(
                sq(coef_b[g]), jnp.concatenate([packed, pltpu.roll(packed, 64, 1)], axis=0)
            )

            @pl.when(g > z)
            def _():
                remote(z_r.at[g], zr_s.at[d], zr_r.at[g], z_peer(d)).wait_recv()

        for d in batch:
            g = (z + d) % GZ
            rhs[g, x] = mm(sq(coef_a[g]), z_r[g]) + mm(sq(through[d]), z_l[g])
        for d in batch:
            g = (z + d) % GZ
            for e in (2, 3, 1):
                send(rhs.at[g, x], w_s.at[d, e], w_r.at[g, x], x_peer(e))

    for d in ARRIVE:
        pieces((d,))

    inner = mm(sq(group_tail), jnp.concatenate([own_follow] + carried, axis=1))
    inner = jnp.concatenate([inner[:, :128] + at_column(group_tail), inner[:, 128:]], axis=1)
    outer = mm(to_exit, inner)
    own_tail = near_tail + outer[:, :128]
    blocks = [base[i] + outer[:, 128 * (i + 1) : 128 * (i + 2)] for i in range(GX)]
    full_r = own_r + mm(sq(own_mt), choose(x, blocks))
    group_mt = choose(z, zf)[:NX]
    group_full = group_r + mm(
        sq(group_mt), choose(x, [inner[:, 128 * (i + 1) : 128 * (i + 2)] for i in range(GX)])
    )
    fac[0] = factors(group_full)
    fac[2] = factors(full_r)
    both = mm(sq(reach), enter) + jnp.where(
        jnp.concatenate([lane, lane], axis=0) == NX, reach, 0.0
    )
    costate = mm(sq(own_tail), both[NX:]) + at_column(own_tail)
    grad_ref[...] = gram[NX : NX + 1, 128:] + jnp.sum(
        both[:NX, NX : NX + 1] * own_r + costate[:, NX : NX + 1] * own_l, axis=0, keepdims=True
    )

    loads[5].wait()
    tile = gram[128:, 128:]
    cost = jnp.concatenate(
        [
            jnp.concatenate([r_v[t], jnp.zeros((NU, 128 - NU), F32)], axis=1)
            if t == 0
            else pltpu.roll(jnp.concatenate([r_v[t], jnp.zeros((NU, 128 - NU), F32)], axis=1), NU * t, 1)
            for t in range(SEC)
        ],
        axis=0,
    )
    for i in range(GX):
        block = rows(fac[jnp.where(i < x, 2, 3)], blocks[i])
        block = block + jnp.where(i == x, tile + cost, 0.0)
        h_ref[:, pl.ds(pl.multiple_of(z * (GX * COLS) + i * COLS, COLS), COLS)] = block

    for batch in [(d,) for d in ARRIVE]:
        for d in batch:
            g = (z + d) % GZ
            for e in range(1, GX):
                i = (x + e) % GX
                remote(rhs.at[g, i], w_s.at[d, e], w_r.at[g, i], x_peer(e)).wait_recv()
        for d in batch:
            g = (z + d) % GZ
            right = jnp.concatenate([rhs[g, i] for i in range(GX)], axis=1)
            if d == ARRIVE[-1]:
                right_ref[...] = right
                left_ref[...] = fac[jnp.where(g > z, 1, 0)].astype(F32)
                continue
            h_ref[:, pl.ds(pl.multiple_of(g * (GX * COLS), GX * COLS), GX * COLS)] = rows(
                fac[jnp.where(g > z, 1, 0)], right
            )

    for copy in sends:
        copy.wait_send()
    for d in Z_ORDER:
        @pl.when((z + d) % GZ < z)
        def _():
            remote(z_r.at[z], zr_s.at[d], zr_r.at[z], z_peer(d)).wait_send()


def settle(h_v, g_v, right_v, left_v, h_out, g_out, last, sem):
    z = lax.axis_index("horizon") // GX
    wide = GX * COLS

    def columns(d):
        return pl.ds(pl.multiple_of(((z + d) % GZ) * wide, wide), wide)

    copies = []
    for d in range(GZ):
        if d != ARRIVE[-1]:
            copies.append(pltpu.make_async_copy(h_v.at[:, columns(d)], h_out.at[0, :, columns(d)], sem.at[d]))
    copies.append(pltpu.make_async_copy(g_v, g_out, sem.at[GZ]))
    for copy in copies:
        copy.start()
    last[...] = rows(left_v[...].astype(BF16), right_v[...])
    copies.append(pltpu.make_async_copy(last, h_out.at[0, :, columns(ARRIVE[-1])], sem.at[ARRIVE[-1]]))
    copies[-1].start()
    for copy in copies:
        copy.wait()


def condense(dynamics, inputs, state_cost, input_cost, drift, target, initial):
    dma = pltpu.SemaphoreType.DMA
    results = pl.pallas_call(
        body,
        out_shape=(
            jax.ShapeDtypeStruct((COLS, GX * GZ * COLS), F32),
            jax.ShapeDtypeStruct((1, COLS), F32),
            jax.ShapeDtypeStruct((NX, GX * COLS), F32),
            jax.ShapeDtypeStruct((COLS, 128), F32),
        ),
        in_specs=[pl.BlockSpec(memory_space=pltpu.HBM)] * 7,
        out_specs=(pl.BlockSpec(memory_space=pltpu.VMEM),) * 4,
        scratch_shapes=[
            pltpu.VMEM((SEC, NX, NX), F32),
            pltpu.VMEM((SEC, NU, NX), F32),
            pltpu.VMEM((SEC, NX, NX), F32),
            pltpu.VMEM((SEC, NU, NU), F32),
            pltpu.VMEM((SEC, NX), F32),
            pltpu.VMEM((SEC, NX), F32),
            pltpu.VMEM((1, NX), F32),
            pltpu.VMEM((SEC * NX, 256), F32),
            pltpu.VMEM((SEC * NX, 256), F32),
            pltpu.VMEM((GX, NX, 128), F32),
            pltpu.VMEM((GX, 2, NX, COLS), F32),
            pltpu.VMEM((GZ, NX, 128), F32),
            pltpu.VMEM((GZ, HALF, 128), F32),
            pltpu.VMEM((GZ, NX, COLS), F32),
            pltpu.VMEM((GZ, NX, COLS), F32),
            pltpu.VMEM((GZ, NX, 128), F32),
            pltpu.VMEM((GZ, NX, 128), F32),
            pltpu.VMEM((GZ, GX, NX, COLS), F32),
            pltpu.VMEM((4, 128, 128), BF16),
            dma((7,)),
            dma((GX,)), dma((GX,)), dma((GX,)), dma((GX,)),
            dma((GZ,)), dma((GZ,)), dma((GZ,)), dma((GZ,)), dma((GZ,)), dma((GZ,)), dma((GZ,)), dma((GZ,)),
            dma((GZ, GX)), dma((GZ, GX)),
        ],
        compiler_params=pltpu.CompilerParams(
            collective_id=0, has_side_effects=True, vmem_limit_bytes=16 * 1024 * 1024
        ),
        name="condense",
    )(*(pltpu.with_memory_space_constraint(v, pltpu.HBM) for v in (dynamics, jnp.swapaxes(inputs, 2, 3), state_cost, input_cost, drift, target, initial)))
    return pl.pallas_call(
        settle,
        out_shape=(
            jax.ShapeDtypeStruct((1, COLS, GX * GZ * COLS), F32),
            jax.ShapeDtypeStruct((1, COLS), F32),
        ),
        in_specs=[pl.BlockSpec(memory_space=pltpu.VMEM)] * 4,
        out_specs=(pl.BlockSpec(memory_space=pltpu.HBM), pl.BlockSpec(memory_space=pltpu.HBM)),
        scratch_shapes=[pltpu.VMEM((COLS, GX * COLS), F32), dma((GZ + 1,))],
        compiler_params=pltpu.CompilerParams(vmem_limit_bytes=4 * 1024 * 1024),
        name="settle",
    )(*results)


def solution(mesh):
    return jax.shard_map(
        condense,
        mesh=mesh,
        in_specs=(
            P("batch", "horizon", None, None),
            P("batch", "horizon", None, None),
            P("batch", "horizon", None, None),
            P("batch", "horizon", None, None),
            P("batch", "horizon", None),
            P("batch", "horizon", None),
            P("batch", None),
        ),
        out_specs=(P("batch", "horizon", None), P("batch", "horizon")),
        check_vma=False,
    )
```
